512 devices in a mesh: orb: 64 (over z, y), fft: 8 (over x, core).
Axes of the slice: x: 4, y: 4, z: 16, core: 2. Of those that a mesh axis runs over, the one named last changes fastest.
Arguments:
- orbitals: bfloat16 [512, 256, 256], P('orb', 'fft'), may hold values from -6 to 6
- kernel: float32 [256, 256], P('fft'), may hold values from 0.02 to 2
- partner_owner: int32 [512, 2, 1], P('orb'), may hold values from 0 to 63; in each aligned block of 16 rows (0 to 15, 16 to 31, ..., all dimensions but the last counted through in order) at most 2 rows name the same one
- partner_local: int32 [512, 2], P('orb'), may hold values from 0 to 7
Outputs:
- exchange_term: float32 [512, 256, 256], P('orb', 'fft')
The draws below stay inside these ranges and needn't reach their ends.
Inputs may be any that keep to these rules, and one draw needn't show every extreme that they name: `partner_owner`: among the 16 partners named on one index of orb, no owner is named more than 2 times, a bound that some block reaches; every owner is named somewhere.
All inputs are finite; a program needn't handle non-finite values.
Results may differ from the reference program's by a relative error of at most 0.0004.
Values may be sent and summed in bfloat16 or wider, within the bound.
No kernel may reach another device: no remote copies, remote signals or barrier semaphores. Data moves between devices by JAX's collectives and lax.ppermute only.
A program may use at most 64 MiB of HBM per device.

```python
import math
import jax
import jax.numpy as jnp
import numpy as np
from jax import lax

GX = 256
GY = 256
ORB_DEV = 8
TASK_DEV = 8
CAP = 2
NORB = 512
TASKS = 512
N_ORB = 64


def place_ends(entries, key, smallest, largest):
    index_at = [jax.random.randint(jax.random.fold_in(key, axis), (), 0, length) for axis, length in enumerate(entries.shape)]
    widest = entries.shape.index(max(entries.shape))
    next_to = index_at[:widest] + [(index_at[widest] + 1) % entries.shape[widest]] + index_at[widest + 1:]
    return entries.at[tuple(index_at)].set(smallest).at[tuple(next_to)].set(largest)


def levels(own_key, dims, cuts, least, largest):
    def one(axis_at, parts):
        draws = jax.random.uniform(jax.random.fold_in(jax.random.fold_in(own_key, 6), axis_at), (parts,), jnp.float32, least / len(cuts), largest / len(cuts))
        return jnp.repeat(jnp.exp(draws), dims[axis_at] // parts).reshape((-1,) + (1,) * (len(dims) - axis_at - 1))

    factor_of = one(*cuts[0])
    for cut in cuts[1:]:
        factor_of = factor_of * one(*cut)
    return factor_of


def routed_block(stream_key, own, number, rows, count, top, bound, slope):
    ranking = jax.random.permutation(stream_key, count)
    packed, usual = load_shares(count, rows * top, bound, slope, True), load_shares(count, rows * top, bound, slope, False)
    places = jnp.arange(count)

    def named(lengths, offset_by):
        used = int((lengths > 0).sum())
        fixed = max(1, used // 4)
        moved = fixed + (places - fixed + offset_by * (used - fixed)) % max(1, count - fixed)
        return jnp.zeros((count,), jnp.int32).at[ranking[jnp.where(places < fixed, places, moved)]].set(jnp.asarray(lengths, jnp.int32))

    lengths = jnp.where(number % 4 == 0, named(packed, number // 4), named(usual, number - number // 4 - 1))
    mixed = jax.random.permutation(jax.random.fold_in(own, 3), count)
    source_of, sink = mixed[0:count // 2 * 2:2], mixed[1:count // 2 * 2:2]
    margin = jnp.minimum(lengths[source_of] - 1, bound - lengths[sink]) // 2
    margin = jnp.where((source_of == ranking[0]) | (sink == ranking[0]) | (lengths[sink] == 0), 0, jnp.maximum(margin, 0))
    moved = jax.random.randint(jax.random.fold_in(own, 4), (count // 2,), 0, 1 << 20) % (margin + 1)
    lengths = lengths.at[source_of].add(-moved).at[sink].add(moved)
    labels = jnp.searchsorted(jnp.cumsum(lengths), jnp.arange(rows * top), side="right").astype(jnp.int32)
    listing = labels.reshape(top, rows).T
    listing = listing[jax.random.permutation(jax.random.fold_in(own, 1), rows)]
    offset_by = jax.random.randint(jax.random.fold_in(own, 2), (rows, 1), 0, top)
    return jnp.take_along_axis(listing, (jnp.arange(top)[None, :] + offset_by) % top, axis=1)


def load_shares(number_of, total, limit, slope, full):
    portions = [(1 << 20) // math.isqrt(standing ** slope) + 1 for standing in range(1, number_of + 1)]
    largest = limit if full else min(limit, max(-(-total // number_of), total * portions[0] // sum(portions)))
    least = 1 if total - largest >= number_of - 1 else 0
    given, spare = [largest] + [least] * (number_of - 1), total - largest - least * (number_of - 1)
    while spare > 0:
        free = [i for i in range(1, number_of) if given[i] < largest] or [i for i in range(1, number_of) if given[i] < limit]
        mass, budget = sum([portions[i] for i in free]), spare
        for i in free:
            extra = min(limit - given[i], max(1, budget * portions[i] // mass), spare)
            given[i] = given[i] + extra
            spare = spare - extra
    return np.array(given)


def centred(own_key, dims, deviation, reach, split=(), dtype=jnp.bfloat16):
    result = deviation * jax.random.normal(own_key, dims, jnp.float32)
    if split:
        result = result * levels(own_key, dims, split, -0.22, 0.18)
    return jnp.clip(result, -reach, reach).astype(dtype)


def setup_inputs(seed: int = 0) -> dict:
    arg_keys = jax.random.split(jax.random.key(seed), 5)
    orbitals = centred(arg_keys[0], (NORB, GX, GY), 1.0, 6.0, ((0, 64), (1, 8)))
    kernel = jnp.clip(jnp.exp(math.log(2.0) - 4.6051702 * jax.random.uniform(arg_keys[1], (GY, GX), jnp.float32) ** levels(arg_keys[1], (GY, GX), ((0, 8),), -0.2, 0.2)), 0.02, 2.0)
    partner_owner_keys = jax.random.split(jax.random.fold_in(arg_keys[2], 1), TASKS * 2 // (2 * TASK_DEV))
    partner_owner_turns = jax.random.permutation(jax.random.fold_in(arg_keys[2], 3), TASKS * 2 // (2 * TASK_DEV))
    partner_owner = jax.vmap(lambda own, number: routed_block(jax.random.fold_in(arg_keys[2], 2), own, number, 2 * TASK_DEV, N_ORB, 1, CAP, 2))(partner_owner_keys, partner_owner_turns).reshape((TASKS, 2, 1))
    partner_local = place_ends(jax.random.randint(arg_keys[3], (TASKS, 2), 0, ORB_DEV), jax.random.fold_in(arg_keys[3], 1), 0, ORB_DEV - 1).astype(jnp.int32)
    return dict(orbitals=orbitals, kernel=kernel, partner_owner=partner_owner, partner_local=partner_local)


def reference(orbitals, kernel, partner_owner, partner_local):
    pair_ids = (partner_owner[:, :, 0] * ORB_DEV + partner_local).astype(jnp.int32)
    blocks = pair_ids.reshape(N_ORB, TASK_DEV, 2)
    weight = kernel.T.astype(jnp.float32)

    def step(total, block):
        first = orbitals[block[:, 0]].astype(jnp.float32)
        second = orbitals[block[:, 1]].astype(jnp.float32)
        density = first * second
        spectrum = jnp.fft.fft2(density, axes=(1, 2))
        potential = jnp.real(jnp.fft.ifft2(spectrum * weight[None], axes=(1, 2))).astype(jnp.float32)
        total = total.at[block[:, 0]].add(potential * second)
        total = total.at[block[:, 1]].add(potential * first)
        return total, None

    start = jnp.zeros((NORB, GX, GY), jnp.float32)
    total, unused = lax.scan(step, start, blocks)
    return -total
```

```python
import math

import jax
import jax.numpy as jnp
import numpy as np
from jax import lax
from jax.experimental import pallas as pl
from jax.experimental.pallas import tpu as pltpu
from jax.sharding import Mesh
from jax.sharding import PartitionSpec as P

Z, Y = 16, 4


def tables(length):
    series = np.arange(length, dtype=np.int64)
    angle = (series[:, None] * series[None, :] % length) * (2.0 * math.pi / length)
    return np.cos(angle).astype(np.float32), np.sin(angle).astype(np.float32)


def halves(a):
    high = a.astype(jnp.bfloat16)
    low = (a - high.astype(jnp.float32)).astype(jnp.bfloat16)
    return high, low


def mul(a, b):
    return jnp.dot(a, b, preferred_element_type=jnp.float32)


def mul3(a, b):
    return mul(a[0], b[0]) + (mul(a[0], b[1]) + mul(a[1], b[0]))


def transform_kernel(grid_ref, weight_ref, cs_high, cs_low, out_ref):
    n = grid_ref.shape[0]
    row = (cs_high[:, :], cs_low[:, :])
    cos = (cs_high[:, :n], cs_low[:, :n])
    sin = (cs_high[:, n:], cs_low[:, n:])
    weight = weight_ref[...].T * (1.0 / (n * n))
    u = halves(mul3(halves(grid_ref[...]), row))
    p = mul3(cos, u)
    q = mul3(sin, u)
    h_real = halves((p[:, :n] - q[:, n:]) * weight)
    h_imag = halves((p[:, n:] + q[:, :n]) * weight)
    g_real = halves(mul3(cos, h_real) + mul3(sin, h_imag))
    g_imag = halves(mul3(sin, h_real) - mul3(cos, h_imag))
    out_ref[...] = mul3(g_real, cos) - mul3(g_imag, sin)


def potential_of(grid, weight):
    n = grid.shape[0]
    both = np.concatenate(tables(n), axis=1)
    high = both.astype(jnp.bfloat16)
    low = (both - high.astype(np.float32)).astype(jnp.bfloat16)
    return pl.pallas_call(
        transform_kernel,
        out_shape=jax.ShapeDtypeStruct((n, n), jnp.float32),
        name="potential",
    )(grid, weight, jnp.asarray(high), jnp.asarray(low))


def swap(x, axis):
    return lax.all_to_all(x, axis, split_axis=0, concat_axis=0, tiled=True)


def on_device(orbitals, kernel, partner_owner, partner_local):
    orb_dev, rows_x, width_y = orbitals.shape
    tasks = partner_local.shape[0]
    fft = lax.axis_size("fft")
    own_y = lax.axis_index("y")
    rows = rows_x // Z
    points = rows * width_y
    lines = orb_dev * points // 128
    named = jnp.concatenate([partner_owner.reshape(-1), partner_local.reshape(-1)])
    named = jnp.pad(named.astype(jnp.bfloat16)[None], ((0, 7), (0, 128 - 4 * tasks)))
    cut = orbitals.reshape(orb_dev, Z, rows, width_y // 128, 128)
    cut = cut.transpose(1, 0, 2, 3, 4).reshape(Z, lines, 128)
    cut = jnp.concatenate([cut, jnp.broadcast_to(named[None], (Z, 8, 128))], axis=1)
    column = swap(cut, "z")
    every = swap(jnp.broadcast_to(column[None], (Y, *column.shape)), "y")
    table = every[:, :, :lines].reshape(Y * Z * orb_dev, points)
    names = column[:, lines, : 4 * tasks].astype(jnp.int32)
    owner = names[:, : 2 * tasks].reshape(Z * tasks, 2)
    local = names[:, 2 * tasks :].reshape(Z * tasks, 2)
    place = (owner % Y) * (Z * orb_dev) + (owner // Y) * orb_dev + local
    place = place.T.reshape(2 * Z * tasks)
    total = Y * Z * orb_dev
    pick = (place[:, None] == jnp.arange(total, dtype=jnp.int32)[None]).astype(jnp.bfloat16)
    chosen = jnp.dot(pick, table, preferred_element_type=jnp.float32)
    left, right = chosen[: Z * tasks], chosen[Z * tasks :]
    density = (left * right).reshape(Z, tasks, points)
    slab = swap(density, "z")
    slab = slab.reshape(Z, tasks, rows, width_y).transpose(1, 0, 2, 3)
    slab = slab.reshape(fft, rows_x, width_y)
    slab = jnp.concatenate([slab, jnp.broadcast_to(kernel[None], (fft, *kernel.shape))], axis=1)
    full = swap(slab, "fft")
    grid = full[:, :rows_x].reshape(fft * rows_x, width_y)
    weight = full[:, rows_x:].reshape(fft * kernel.shape[0], kernel.shape[1])
    spread = potential_of(grid, weight).reshape(fft, rows_x, width_y)
    back = swap(spread, "fft")
    back = back.reshape(tasks, Z, rows, width_y).transpose(1, 0, 2, 3).reshape(Z, tasks, points)
    potential = swap(back, "z").reshape(Z * tasks, points)
    contrib = jnp.concatenate([potential * right, potential * left], axis=0)
    place_hot = (jnp.arange(total, dtype=jnp.int32)[:, None] == place[None]).astype(jnp.float32)
    summed = -jnp.dot(place_hot, contrib, precision=lax.Precision.HIGHEST)
    summed = swap(summed.reshape(Y, Z * orb_dev, points), "y").sum(0)
    home = swap(summed.reshape(Z, orb_dev, points), "z")
    home = home.reshape(Z, orb_dev, rows, width_y).transpose(1, 0, 2, 3)
    return home.reshape(orb_dev, rows_x, width_y)


def solution(mesh):
    devices = mesh.devices.reshape(Z, Y, mesh.devices.shape[1])
    fine = Mesh(devices, ("z", "y", "fft"))
    orb = ("z", "y")
    in_specs = (P(orb, "fft", None), P("fft", None), P(orb, None, None), P(orb, None))
    out_specs = P(orb, "fft", None)
    return jax.shard_map(
        on_device, mesh=fine, in_specs=in_specs, out_specs=out_specs, check_vma=False
    )
```

```python
import math

import jax
import jax.numpy as jnp
import numpy as np
from jax import lax
from jax.experimental import pallas as pl
from jax.experimental.pallas import tpu as pltpu
from jax.sharding import Mesh
from jax.sharding import PartitionSpec as P

Z, Y = 16, 4
LANES = 128
TOP = 32767.0
STEPS = 128.0
FLOOR = 1e-37
KERNEL_LOW, KERNEL_HIGH = 0.02, 2.0
KERNEL_MID = 0.5 * (math.log(KERNEL_HIGH) + math.log(KERNEL_LOW))
KERNEL_STEP = 0.5 * (math.log(KERNEL_HIGH) - math.log(KERNEL_LOW)) / TOP


def tables(length):
    series = np.arange(length, dtype=np.int64)
    angle = (series[:, None] * series[None, :] % length) * (2.0 * math.pi / length)
    return np.cos(angle).astype(np.float32), np.sin(angle).astype(np.float32)


def level_of(largest):
    return jnp.ceil(jnp.log(jnp.maximum(largest, FLOOR)) * (STEPS / math.log(2.0))) + 1.0


def coded(values, level):
    share = jnp.sqrt(jnp.abs(values) * jnp.exp(level * (-math.log(2.0) / STEPS)))
    share = jnp.round(jnp.minimum(share, 1.0) * TOP)
    return jnp.where(values < 0, -share, share)


def decoded(codes, level):
    share = codes * (1.0 / TOP)
    return share * jnp.abs(share) * jnp.exp(level * (math.log(2.0) / STEPS))


def to_16(codes):
    return codes.astype(jnp.int32).astype(jnp.int16)


def from_16(codes):
    return codes.astype(jnp.int32).astype(jnp.float32)


def coded_rows(values):
    level = level_of(jnp.max(jnp.abs(values), axis=1, keepdims=True))
    behind = jnp.broadcast_to(level, (values.shape[0], LANES))
    return to_16(jnp.concatenate([coded(values, level), behind], axis=1))


def decoded_rows(codes, points):
    wide = from_16(codes)
    return decoded(wide[..., :points], wide[..., points : points + 1])


def halves(a):
    high = a.astype(jnp.bfloat16)
    low = (a - high.astype(jnp.float32)).astype(jnp.bfloat16)
    return high, low


def mul(a, b):
    return jnp.dot(a, b, preferred_element_type=jnp.float32)


def mul3(a, b):
    return mul(a[0], b[0]) + (mul(a[0], b[1]) + mul(a[1], b[0]))


def transform_kernel(data_ref, cs_high, cs_low, out_ref):
    n = data_ref.shape[2]
    slabs = data_ref.shape[0]
    rows = n // slabs
    data = from_16(data_ref[...])
    level = data[:, rows : rows + 8][:, None]
    grid = decoded(data[:, :rows].reshape(slabs, rows // 8, 8, n), level).reshape(n, n)
    weight = jnp.exp(data[:, rows + 8 :].reshape(n, n) * KERNEL_STEP + KERNEL_MID)
    weight = weight.T * (1.0 / (n * n))
    row = (cs_high[:, :], cs_low[:, :])
    cos = (cs_high[:, :n], cs_low[:, :n])
    sin = (cs_high[:, n:], cs_low[:, n:])
    u = halves(mul3(halves(grid), row))
    p = mul3(cos, u)
    q = mul3(sin, u)
    h_real = halves((p[:, :n] - q[:, n:]) * weight)
    h_imag = halves((p[:, n:] + q[:, :n]) * weight)
    g_real = halves(mul3(cos, h_real) + mul3(sin, h_imag))
    g_imag = halves(mul3(sin, h_real) - mul3(cos, h_imag))
    spread = mul3(g_real, cos) - mul3(g_imag, sin)
    level = level_of(jnp.max(jnp.abs(spread), axis=(0, 1), keepdims=True))
    codes = coded(spread, level).reshape(slabs, rows, n)
    behind = jnp.broadcast_to(level[None], (slabs, 8, n))
    out_ref[...] = to_16(jnp.concatenate([codes, behind], axis=1))


def potential_of(data):
    slabs, height, n = data.shape
    both = np.concatenate(tables(n), axis=1)
    high = both.astype(jnp.bfloat16)
    low = (both - high.astype(np.float32)).astype(jnp.bfloat16)
    return pl.pallas_call(
        transform_kernel,
        out_shape=jax.ShapeDtypeStruct((slabs, n // slabs + 8, n), jnp.int16),
        name="potential",
    )(data, jnp.asarray(high), jnp.asarray(low))


def swap(x, axis):
    return lax.all_to_all(x, axis, split_axis=0, concat_axis=0, tiled=True)


def to_all(x, axis):
    return swap(jnp.broadcast_to(x[None], (lax.axis_size(axis), *x.shape)), axis)


def pieces(slab):
    count, rows, width = slab.shape
    cut = slab.reshape(count, rows // 8, 8, width // LANES, LANES).transpose(2, 3, 0, 1, 4)
    return cut.reshape(Z, count, rows // 8 * LANES)


def whole(cut, width):
    count = cut.shape[1]
    slab = cut.reshape(8, width // LANES, count, -1, LANES).transpose(2, 3, 0, 1, 4)
    return slab.reshape(count, -1, width)


def on_device(orbitals, kernel, partner_owner, partner_local):
    orb_dev, rows_x, width_y = orbitals.shape
    tasks = partner_local.shape[0]
    points = rows_x * width_y // Z
    total = Y * Z * orb_dev
    own_y = lax.axis_index("y")
    named = jnp.concatenate([partner_owner[:, :, 0], partner_local], axis=1)
    named = jnp.pad(named.astype(jnp.bfloat16), ((0, 0), (0, LANES - 4)))
    behind = jnp.broadcast_to(named[None], (Z, tasks, LANES))
    column = swap(jnp.concatenate([pieces(orbitals), behind], axis=2), "z")
    every = to_all(column, "y").reshape(total, points + LANES)
    table = every[:, :points]

    def places(block):
        names = block[:, points : points + 4].astype(jnp.int32)
        owner = names[:, :2].T.reshape(-1)
        return (owner % Y * Z + owner // Y) * orb_dev + names[:, 2:].T.reshape(-1)

    def chosen(place):
        pick = place[:, None] == jnp.arange(total, dtype=jnp.int32)[None]
        return mul(pick.astype(jnp.bfloat16), table)

    own = chosen(places(column.reshape(Z * tasks, points + LANES)))
    density = coded_rows(own[: Z * tasks] * own[Z * tasks :])
    slab = whole(swap(density.reshape(Z, tasks, -1), "z"), width_y)
    weight = to_16(jnp.round((jnp.log(kernel) - KERNEL_MID) * (1.0 / KERNEL_STEP)))
    weight = jnp.broadcast_to(weight[None], (tasks, *weight.shape))
    full = swap(jnp.concatenate([slab, weight], axis=1), "fft")
    back = swap(potential_of(full), "fft")
    spread = to_all(swap(pieces(back), "z"), "y").reshape(total, -1)
    place = places(every)
    partner = chosen(jnp.concatenate([place[total:], place[:total]]))
    potential = decoded_rows(spread, points)
    contrib = (partner.reshape(2, total, points) * potential[None]).reshape(2 * total, points)
    mine = jnp.arange(Z * orb_dev, dtype=jnp.int32) + own_y * (Z * orb_dev)
    select = (mine[:, None] == place[None]).astype(jnp.bfloat16)
    high = lax.reduce_precision(contrib, 8, 7)
    low = (contrib - high).astype(jnp.bfloat16)
    summed = mul(select, high.astype(jnp.bfloat16)) + mul(select, low)
    home = swap(coded_rows(-summed).reshape(Z, orb_dev, -1), "z")
    return whole(decoded_rows(home, points), width_y)


def solution(mesh):
    devices = mesh.devices.reshape(Z, Y, mesh.devices.shape[1])
    fine = Mesh(devices, ("z", "y", "fft"))
    orb = ("z", "y")
    in_specs = (P(orb, "fft", None), P("fft", None), P(orb, None, None), P(orb, None))
    out_specs = P(orb, "fft", None)
    return jax.shard_map(
        on_device, mesh=fine, in_specs=in_specs, out_specs=out_specs, check_vma=False
    )
```

```python
import math

import jax
import jax.numpy as jnp
import numpy as np
from jax import lax
from jax.experimental import pallas as pl
from jax.experimental.pallas import tpu as pltpu
from jax.sharding import Mesh
from jax.sharding import PartitionSpec as P

Z, Y = 16, 4
LANES = 128
TOP = 32767.0
STEPS = 128.0
FLOOR = 1e-37
KERNEL_LOW, KERNEL_HIGH = 0.02, 2.0
KERNEL_MID = 0.5 * (math.log(KERNEL_HIGH) + math.log(KERNEL_LOW))
KERNEL_STEP = 0.5 * (math.log(KERNEL_HIGH) - math.log(KERNEL_LOW)) / TOP


def tables(length):
    series = np.arange(length, dtype=np.int64)
    angle = (series[:, None] * series[None, :] % length) * (2.0 * math.pi / length)
    return np.cos(angle).astype(np.float32), np.sin(angle).astype(np.float32)


def level_of(largest):
    return jnp.ceil(jnp.log(jnp.maximum(largest, FLOOR)) * (STEPS / math.log(2.0))) + 1.0


def coded(values, level):
    share = jnp.sqrt(jnp.abs(values) * jnp.exp(level * (-math.log(2.0) / STEPS)))
    share = jnp.round(jnp.minimum(share, 1.0) * TOP)
    return jnp.where(values < 0, -share, share)


def decoded(codes, level):
    share = codes * (1.0 / TOP)
    return share * jnp.abs(share) * jnp.exp(level * (math.log(2.0) / STEPS))


def to_16(codes):
    return codes.astype(jnp.int32).astype(jnp.int16)


def from_16(codes):
    return codes.astype(jnp.int32).astype(jnp.float32)


def coded_rows(values):
    level = level_of(jnp.max(jnp.abs(values), axis=1, keepdims=True))
    behind = jnp.broadcast_to(level, (values.shape[0], LANES))
    return to_16(jnp.concatenate([coded(values, level), behind], axis=1))


def decoded_rows(codes, points):
    wide = from_16(codes)
    return decoded(wide[..., :points], wide[..., points + 4 : points + 5])


def halves(a):
    high = a.astype(jnp.bfloat16)
    low = (a - high.astype(jnp.float32)).astype(jnp.bfloat16)
    return high, low


def mul(a, b):
    return jnp.dot(a, b, preferred_element_type=jnp.float32)


def mul3(a, b):
    return mul(a[0], b[0]) + (mul(a[0], b[1]) + mul(a[1], b[0]))


def transform_kernel(data_ref, cs_high, cs_low, out_ref):
    n = data_ref.shape[2]
    slabs = data_ref.shape[0]
    rows = n // slabs
    data = from_16(data_ref[...])
    level = data[:, rows : rows + 8][:, None]
    grid = decoded(data[:, :rows].reshape(slabs, rows // 8, 8, n), level).reshape(n, n)
    weight = jnp.exp(data[:, rows + 8 :].reshape(n, n) * KERNEL_STEP + KERNEL_MID)
    weight = weight.T * (1.0 / (n * n))
    row = (cs_high[:, :], cs_low[:, :])
    cos = (cs_high[:, :n], cs_low[:, :n])
    sin = (cs_high[:, n:], cs_low[:, n:])
    u = halves(mul3(halves(grid), row))
    p = mul3(cos, u)
    q = mul3(sin, u)
    h_real = halves((p[:, :n] - q[:, n:]) * weight)
    h_imag = halves((p[:, n:] + q[:, :n]) * weight)
    g_real = halves(mul3(cos, h_real) + mul3(sin, h_imag))
    g_imag = halves(mul3(sin, h_real) - mul3(cos, h_imag))
    spread = mul3(g_real, cos) - mul3(g_imag, sin)
    level = level_of(jnp.max(jnp.abs(spread), axis=(0, 1), keepdims=True))
    codes = coded(spread, level).reshape(slabs, rows, n)
    behind = jnp.broadcast_to(level[None], (slabs, 8, n))
    out_ref[...] = to_16(jnp.concatenate([codes, behind], axis=1))


def potential_of(data):
    slabs, height, n = data.shape
    both = np.concatenate(tables(n), axis=1)
    high = both.astype(jnp.bfloat16)
    low = (both - high.astype(np.float32)).astype(jnp.bfloat16)
    return pl.pallas_call(
        transform_kernel,
        out_shape=jax.ShapeDtypeStruct((slabs, n // slabs + 8, n), jnp.int16),
        name="potential",
    )(data, jnp.asarray(high), jnp.asarray(low))


def swap(x, axis):
    return lax.all_to_all(x, axis, split_axis=0, concat_axis=0, tiled=True)


def to_all(x, axis):
    return lax.all_gather(x, axis, axis=0, tiled=False)


def pieces(slab):
    count, rows, width = slab.shape
    cut = slab.reshape(count, rows // 8, 8, width // LANES, LANES).transpose(2, 3, 0, 1, 4)
    return cut.reshape(Z, count, rows // 8 * LANES)


def whole(cut, width):
    count = cut.shape[1]
    slab = cut.reshape(8, width // LANES, count, -1, LANES).transpose(2, 3, 0, 1, 4)
    return slab.reshape(count, -1, width)


def on_device(orbitals, kernel, partner_owner, partner_local):
    orb_dev, rows_x, width_y = orbitals.shape
    tasks = partner_local.shape[0]
    points = rows_x * width_y // Z
    total = Y * Z * orb_dev
    own_y = lax.axis_index("y")
    named = jnp.concatenate([partner_owner[:, :, 0], partner_local], axis=1)
    named = jnp.pad(named.astype(jnp.bfloat16), ((0, 0), (0, LANES - 4)))
    behind = jnp.broadcast_to(named[None], (Z, tasks, LANES))
    column = swap(jnp.concatenate([pieces(orbitals), behind], axis=2), "z")
    table = to_all(column[:, :, :points], "y").reshape(total, points)

    def places(block):
        names = block.reshape(-1, points + LANES)[:, points : points + 4].astype(jnp.int32)
        owner = names[:, :2].T.reshape(-1)
        return (owner % Y * Z + owner // Y) * orb_dev + names[:, 2:].T.reshape(-1)

    def chosen(place):
        pick = place[:, None] == jnp.arange(total, dtype=jnp.int32)[None]
        return mul(pick.astype(jnp.bfloat16), table)

    own = chosen(places(column))
    density = coded_rows(own[: Z * tasks] * own[Z * tasks :])
    slab = whole(swap(density.reshape(Z, tasks, -1), "z"), width_y)
    weight = to_16(jnp.round((jnp.log(kernel) - KERNEL_MID) * (1.0 / KERNEL_STEP)))
    weight = jnp.broadcast_to(weight[None], (tasks, *weight.shape))
    full = swap(jnp.concatenate([slab, weight], axis=1), "fft")
    back = swap(potential_of(full), "fft")
    spread = swap(pieces(back), "z")
    lane = jnp.arange(points + LANES, dtype=jnp.int32)
    beside = (lane >= points) & (lane < points + 4)
    spread = to_all(jnp.where(beside, column.astype(jnp.int16), spread), "y")
    place = places(spread)
    partner = chosen(jnp.concatenate([place[total:], place[:total]]))
    potential = decoded_rows(spread.reshape(total, -1), points)
    contrib = (partner.reshape(2, total, points) * potential[None]).reshape(2 * total, points)
    mine = jnp.arange(Z * orb_dev, dtype=jnp.int32) + own_y * (Z * orb_dev)
    select = (mine[:, None] == place[None]).astype(jnp.bfloat16)
    high = lax.reduce_precision(contrib, 8, 7)
    low = (contrib - high).astype(jnp.bfloat16)
    summed = mul(select, high.astype(jnp.bfloat16)) + mul(select, low)
    home = swap(coded_rows(-summed).reshape(Z, orb_dev, -1), "z")
    return whole(decoded_rows(home, points), width_y)


def solution(mesh):
    devices = mesh.devices.reshape(Z, Y, mesh.devices.shape[1])
    fine = Mesh(devices, ("z", "y", "fft"))
    orb = ("z", "y")
    in_specs = (P(orb, "fft", None), P("fft", None), P(orb, None, None), P(orb, None))
    out_specs = P(orb, "fft", None)
    return jax.shard_map(
        on_device, mesh=fine, in_specs=in_specs, out_specs=out_specs, check_vma=False
    )
```

```python
import math

import jax
import jax.numpy as jnp
import numpy as np
from jax import lax
from jax.experimental import pallas as pl
from jax.experimental.pallas import tpu as pltpu
from jax.sharding import Mesh
from jax.sharding import PartitionSpec as P

Z, Y = 16, 4
LANES = 128
TOP = 32767.0
STEPS = 128.0
FLOOR = 1e-37
KERNEL_LOW, KERNEL_HIGH = 0.02, 2.0
KERNEL_MID = 0.5 * (math.log(KERNEL_HIGH) + math.log(KERNEL_LOW))
KERNEL_STEP = 0.5 * (math.log(KERNEL_HIGH) - math.log(KERNEL_LOW)) / TOP


def tables(length):
    series = np.arange(length, dtype=np.int64)
    angle = (series[:, None] * series[None, :] % length) * (2.0 * math.pi / length)
    return np.cos(angle).astype(np.float32), np.sin(angle).astype(np.float32)


def level_of(largest):
    return jnp.ceil(jnp.log(jnp.maximum(largest, FLOOR)) * (STEPS / math.log(2.0))) + 1.0


def coded(values, level):
    share = jnp.sqrt(jnp.abs(values) * jnp.exp(level * (-math.log(2.0) / STEPS)))
    share = jnp.round(jnp.minimum(share, 1.0) * TOP)
    return jnp.where(values < 0, -share, share)


def decoded(codes, level):
    share = codes * (1.0 / TOP)
    return share * jnp.abs(share) * jnp.exp(level * (math.log(2.0) / STEPS))


def to_16(codes):
    return codes.astype(jnp.int32).astype(jnp.int16)


def from_16(codes):
    return codes.astype(jnp.int32).astype(jnp.float32)


def halves(a):
    high = a.astype(jnp.bfloat16)
    low = (a - high.astype(jnp.float32)).astype(jnp.bfloat16)
    return high, low


def mul(a, b):
    return jnp.dot(a, b, preferred_element_type=jnp.float32)


def mul3(a, b):
    return mul(a[0], b[0]) + (mul(a[0], b[1]) + mul(a[1], b[0]))


def transform_kernel(data_ref, cs_high, cs_low, out_ref):
    n = cs_high.shape[0]
    count, _, lanes = data_ref.shape
    depth = n * n // (count * lanes)
    halved = n // lanes

    def assembled(blocks):
        blocks = blocks.reshape(Y // halved, halved, count // Y, depth, lanes)
        sides = [
            jnp.concatenate(
                [blocks[upper, side][:, None] for upper in range(Y // halved)], axis=1
            ).reshape(n, lanes)
            for side in range(halved)
        ]
        return jnp.concatenate(sides, axis=1)

    codes = from_16(data_ref[:, :depth])
    level = from_16(data_ref[:, depth : 2 * depth])
    grid = assembled(decoded(codes, level))
    log_weight = assembled(from_16(data_ref[:, 2 * depth :]))
    weight = jnp.exp(log_weight * KERNEL_STEP + KERNEL_MID).T * (1.0 / (n * n))
    row = (cs_high[:, :], cs_low[:, :])
    cos = (cs_high[:, :n], cs_low[:, :n])
    sin = (cs_high[:, n:], cs_low[:, n:])
    u = halves(mul3(halves(grid), row))
    p = mul3(cos, u)
    q = mul3(sin, u)
    h_real = halves((p[:, :n] - q[:, n:]) * weight)
    h_imag = halves((p[:, n:] + q[:, :n]) * weight)
    g_real = halves(mul3(cos, h_real) + mul3(sin, h_imag))
    g_imag = halves(mul3(sin, h_real) - mul3(cos, h_imag))
    spread = mul3(g_real, cos) - mul3(g_imag, sin)
    level = level_of(jnp.max(jnp.abs(spread), axis=(0, 1), keepdims=True))
    codes = coded(spread, level).reshape(count // Y, Y // halved, depth, n)
    out_ref[:, depth:] = to_16(jnp.broadcast_to(level[None], (count, 8, lanes)))
    for upper in range(Y // halved):
        for side in range(halved):
            part = codes[:, upper, :, side * lanes : (side + 1) * lanes]
            start = (upper * halved + side) * (count // Y)
            out_ref[start : start + count // Y, :depth] = to_16(part)


def potential_of(data, n):
    count, height, lanes = data.shape
    both = np.concatenate(tables(n), axis=1)
    high = both.astype(jnp.bfloat16)
    low = (both - high.astype(np.float32)).astype(jnp.bfloat16)
    return pl.pallas_call(
        transform_kernel,
        out_shape=jax.ShapeDtypeStruct((count, height // 3 + 8, lanes), jnp.int16),
        name="potential",
    )(data, jnp.asarray(high), jnp.asarray(low))


def swap(x, axis):
    return lax.all_to_all(x, axis, split_axis=0, concat_axis=0, tiled=True)


def paired(codes, tail):
    n, rows, lanes = codes.shape
    tail = jnp.pad(tail, ((0, 0), (0, 0), (0, lanes - tail.shape[2])))
    return jnp.concatenate([codes.reshape(n, rows // 2, 2, lanes), tail[:, None]], axis=1)


def row_level(values):
    return level_of(jnp.max(jnp.abs(values), axis=-1, keepdims=True))


def with_levels(codes, level):
    n, rows, _ = codes.shape
    tail = level.reshape(n, rows // 2, 2).transpose(0, 2, 1)
    return paired(to_16(codes), to_16(tail))


def levels_of(message):
    n, pairs = message.shape[0], message.shape[1] - 1
    tail = message[:, pairs, :, :pairs].transpose(0, 2, 1)
    return tail.reshape(n, pairs * 2)


def codes_of(message):
    n, pairs, _, lanes = message.shape
    return message[:, : pairs - 1].reshape(n, (pairs - 1) * 2, lanes)


def on_device(orbitals, kernel, partner_owner, partner_local):
    orb_dev, rows_x, width_y = orbitals.shape
    tasks = partner_local.shape[0]
    peers = Z * Y
    total = peers * orb_dev
    fft = lax.axis_size("fft")
    sides = width_y // LANES
    cut = orbitals.reshape(orb_dev, Y // sides, Z, sides, LANES).transpose(2, 1, 3, 0, 4)
    named = jnp.concatenate([partner_owner[:, :, 0].T, partner_local.T], axis=1)
    named = jnp.broadcast_to(named.astype(jnp.bfloat16)[None], (peers, 2, 2 * tasks))
    first = swap(paired(cut.reshape(peers, orb_dev, LANES), named), ("z", "y"))
    table = codes_of(first).reshape(total, LANES)
    names = first[:, orb_dev // 2, :, : 2 * tasks].astype(jnp.int32)
    place = names[:, :, :tasks] * orb_dev + names[:, :, tasks:]
    place = place.transpose(1, 0, 2).reshape(2 * total)
    orbs = jnp.arange(total, dtype=jnp.int32)
    pick = (place[:, None] == orbs[None]).astype(jnp.bfloat16)
    chosen = mul(pick, table)
    left, right = chosen[:total], chosen[total:]
    density = left * right
    level = row_level(density)
    block = Y * tasks
    there = with_levels(coded(density, level).reshape(Z, block, LANES), level)
    there = swap(there, "z")
    codes = codes_of(there).transpose(1, 0, 2)
    level = jnp.broadcast_to(levels_of(there).T[:, :, None], codes.shape)
    weight = to_16(jnp.round((jnp.log(kernel) - KERNEL_MID) * (1.0 / KERNEL_STEP)))
    weight = weight.reshape(Y // sides, Z, sides, LANES).transpose(0, 2, 1, 3)
    own_y = lax.axis_index("y")
    weight = lax.dynamic_index_in_dim(weight.reshape(Y, Z, LANES), own_y, 0)
    weight = jnp.broadcast_to(weight, codes.shape)
    data = swap(jnp.concatenate([codes, level, weight], axis=1), ("y", "fft"))
    back = swap(potential_of(data, width_y), ("y", "fft"))
    level = jnp.broadcast_to(back[None, :, Z, :1], (Z, block, 1))
    codes = back[:, :Z].transpose(1, 0, 2)
    tail = level.reshape(Z, block // 2, 2).transpose(0, 2, 1)
    spread = swap(paired(codes, tail), "z")
    level = from_16(levels_of(spread)).reshape(total, 1)
    potential = decoded(from_16(codes_of(spread)).reshape(total, LANES), level)
    contrib = jnp.concatenate([potential * right, potential * left], axis=0)
    select = (orbs[:, None] == place[None]).astype(jnp.bfloat16)
    high = lax.reduce_precision(contrib, 8, 7)
    low = (contrib - high).astype(jnp.bfloat16)
    summed = -(mul(select, high.astype(jnp.bfloat16)) + mul(select, low))
    level = row_level(summed)
    home = with_levels(coded(summed, level).reshape(peers, orb_dev, LANES), level)
    home = swap(home, ("z", "y"))
    level = from_16(levels_of(home))[:, :, None]
    result = decoded(from_16(codes_of(home)), level)
    result = result.reshape(Z, Y // sides, sides, orb_dev, LANES).transpose(3, 1, 0, 2, 4)
    return result.reshape(orb_dev, rows_x, width_y)


def solution(mesh):
    devices = mesh.devices.reshape(Z, Y, mesh.devices.shape[1])
    fine = Mesh(devices, ("z", "y", "fft"))
    orb = ("z", "y")
    in_specs = (P(orb, "fft", None), P("fft", None), P(orb, None, None), P(orb, None))
    out_specs = P(orb, "fft", None)
    return jax.shard_map(
        on_device, mesh=fine, in_specs=in_specs, out_specs=out_specs, check_vma=False
    )
```

```python
import math

import jax
import jax.numpy as jnp
import numpy as np
from jax import lax
from jax.experimental import pallas as pl
from jax.experimental.pallas import tpu as pltpu
from jax.sharding import Mesh
from jax.sharding import PartitionSpec as P

Z, Y = 16, 4
LANES = 128
TOP = 32767.0
STEPS = 128.0
FLOOR = 1e-37
KERNEL_LOW, KERNEL_HIGH = 0.02, 2.0
KERNEL_MID = 0.5 * (math.log(KERNEL_HIGH) + math.log(KERNEL_LOW))
KERNEL_STEP = 0.5 * (math.log(KERNEL_HIGH) - math.log(KERNEL_LOW)) / TOP


def tables(length):
    series = np.arange(length, dtype=np.int64)
    angle = (series[:, None] * series[None, :] % length) * (2.0 * math.pi / length)
    return np.cos(angle).astype(np.float32), np.sin(angle).astype(np.float32)


def level_of(largest):
    return jnp.ceil(jnp.log(jnp.maximum(largest, FLOOR)) * (STEPS / math.log(2.0))) + 1.0


def coded(values, level):
    share = jnp.sqrt(jnp.abs(values) * jnp.exp(level * (-math.log(2.0) / STEPS)))
    share = jnp.round(jnp.minimum(share, 1.0) * TOP)
    return jnp.where(values < 0, -share, share)


def decoded(codes, level):
    share = codes * (1.0 / TOP)
    return share * jnp.abs(share) * jnp.exp(level * (math.log(2.0) / STEPS))


def to_16(codes):
    return codes.astype(jnp.int32).astype(jnp.int16)


def from_16(codes):
    return codes.astype(jnp.int32).astype(jnp.float32)


def halves(a):
    high = a.astype(jnp.bfloat16)
    low = (a - high.astype(jnp.float32)).astype(jnp.bfloat16)
    return high, low


def mul(a, b):
    return jnp.dot(a, b, preferred_element_type=jnp.float32)


def mul3(a, b):
    return mul(a[0], b[0]) + (mul(a[0], b[1]) + mul(a[1], b[0]))


def lane_of(shape):
    return lax.broadcasted_iota(jnp.int32, shape, len(shape) - 1)


def row_level(values):
    return level_of(jnp.max(jnp.abs(values), axis=-1, keepdims=True))


def to_lanes(level, n):
    rows, lanes = level.shape
    split = level.reshape(n, rows // n // 2, 2, lanes)
    pair = lax.broadcasted_iota(jnp.int32, split.shape, 1)
    return jnp.sum(jnp.where(lane_of(split.shape) == pair, split, 0.0), axis=1)


def to_rows(tail, pairs):
    n, _, lanes = tail.shape
    rows = 2 * pairs
    spread = jnp.broadcast_to(tail[:, None], (n, pairs, 2, lanes)).reshape(n, rows, lanes)
    row = lax.broadcasted_iota(jnp.int32, spread.shape, 1)
    kept = jnp.where(lane_of(spread.shape) == row // 2, spread, 0.0)
    return jnp.sum(kept.reshape(n * rows, lanes), axis=1, keepdims=True)


def write_rows(out_ref, values):
    n, pairs = out_ref.shape[0], out_ref.shape[1] - 1
    lanes = values.shape[1]
    level = row_level(values)
    codes = coded(values, level)
    out_ref[:, :pairs] = to_16(codes.reshape(n, pairs, 2, lanes))
    wide = jnp.broadcast_to(level, values.shape)
    out_ref[:, pairs:] = to_16(to_lanes(wide, n)[:, None])


def read_rows(ref):
    n, pairs, lanes = ref.shape[0], ref.shape[1] - 1, ref.shape[3]
    codes = from_16(ref[:, :pairs]).reshape(n * pairs * 2, lanes)
    return decoded(codes, to_rows(from_16(ref[:, pairs]), pairs))


def pack_kernel(orb_ref, owner_ref, local_ref, out_ref):
    count, rows, width = orb_ref.shape
    half = rows // Z
    orbs = orb_ref[...].astype(jnp.float32)
    for side in range(width // LANES):
        part = jnp.swapaxes(orbs[:, :, side * LANES : (side + 1) * LANES], 0, 1)
        for upper in range(half):
            piece = part[upper * Z : (upper + 1) * Z].reshape(Z, count // 2, 2, LANES)
            out_ref[:, upper, side, : count // 2] = piece.astype(jnp.bfloat16)
    lane = lane_of((local_ref.shape[0], LANES))
    task = lax.broadcasted_iota(jnp.int32, lane.shape, 0)
    rows_of = []
    for c in range(2):
        names = owner_ref[:, c] * count + local_ref[:, c : c + 1] - 256
        spread = jnp.where(lane == task, jnp.broadcast_to(names, lane.shape), 0)
        rows_of.append(jnp.sum(spread.astype(jnp.float32), axis=0, keepdims=True))
    tail = jnp.concatenate(rows_of, axis=0).astype(jnp.bfloat16)
    shape = (Z, half, width // LANES, 1, 2, LANES)
    out_ref[:, :, :, count // 2 :] = jnp.broadcast_to(tail[None, None, None, None], shape)


def density_kernel(first_ref, there_ref, chosen_ref, place_ref):
    peers, pairs, _, lanes = first_ref.shape
    pairs = pairs - 1
    total = peers * pairs * 2
    table = first_ref[:, :pairs].astype(jnp.float32).reshape(total, lanes)
    tasks = total // peers
    group = lanes // tasks
    tails = first_ref[:, pairs].astype(jnp.float32).reshape(peers // group, group, 2, lanes)
    place = tails[:, 0]
    for s in range(1, group):
        place = place + pltpu.roll(tails[:, s], s * tasks, 2)
    place = place.reshape(2 * (peers // group), lanes) + 256.0
    place_ref[...] = place
    column = place.T
    orbs = lane_of((lanes, total)).astype(jnp.float32)
    sides = []
    for c in range(2):
        pick = [
            (orbs == column[:, 2 * j + c : 2 * j + c + 1]).astype(jnp.bfloat16)
            for j in range(total // lanes)
        ]
        sides.append(mul(jnp.concatenate(pick, axis=0), table.astype(jnp.bfloat16)))
        chosen_ref[c] = sides[c].astype(jnp.bfloat16)
    write_rows(there_ref, sides[0] * sides[1])


def onward_kernel(place_ref, there_ref, weight_ref, out_ref):
    depth, pairs, _, lanes = there_ref.shape
    pairs = pairs - 1
    block = 2 * pairs
    half = depth // 2
    codes = from_16(there_ref[:, :pairs]).reshape(depth, block, lanes)
    codes = jnp.swapaxes(codes, 0, 1).reshape(block, half, 2, lanes)
    out_ref[:, :half] = to_16(codes)
    level = from_16(there_ref[:, pairs]).reshape(2 * depth, lanes).T[:pairs]
    level = jnp.concatenate([level, jnp.zeros((pairs, lanes - 2 * depth), jnp.float32)], axis=1)
    level = jnp.broadcast_to(level[:, None, None], (pairs, 2, 2, lanes)).reshape(block, 2, lanes)
    out_ref[:, 2 * half :] = to_16(level[:, None])
    own = jnp.zeros((depth, lanes), jnp.float32)
    for upper in range(weight_ref.shape[0] // depth):
        for side in range(weight_ref.shape[1] // lanes):
            part = weight_ref[upper * depth : (upper + 1) * depth, side * lanes : (side + 1) * lanes]
            here = place_ref[0] == upper * (weight_ref.shape[1] // lanes) + side
            own = jnp.where(here, part, own)
    own = jnp.round((jnp.log(own) - KERNEL_MID) * (1.0 / KERNEL_STEP)).reshape(half, 2, lanes)
    out_ref[:, half : 2 * half] = jnp.broadcast_to(to_16(own)[None], (block, half, 2, lanes))


def transform_kernel(place_ref, data_ref, cs_high, cs_low, out_ref):
    n = cs_high.shape[0]
    count, _, _, lanes = data_ref.shape
    depth = n * n // (count * lanes)
    half = depth // 2
    halved = n // lanes

    def assembled(blocks):
        blocks = blocks.reshape(Y // halved, halved, count // Y, depth, lanes)
        sides = [
            jnp.concatenate(
                [blocks[upper, side][:, None] for upper in range(Y // halved)], axis=1
            ).reshape(n, lanes)
            for side in range(halved)
        ]
        return jnp.concatenate(sides, axis=1)

    codes = from_16(data_ref[:, :half]).reshape(count, depth, lanes)
    tail = from_16(data_ref[:, 2 * half, :1])
    tail = jnp.broadcast_to(tail, (count, depth, lanes))
    row = lax.broadcasted_iota(jnp.int32, tail.shape, 1)
    tail = jnp.where(lane_of(tail.shape) == 2 * row + place_ref[1], tail, 0.0)
    grid = assembled(decoded(codes, jnp.sum(tail, axis=2, keepdims=True)))
    log_weight = assembled(from_16(data_ref[:, half : 2 * half]).reshape(count, depth, lanes))
    weight = jnp.exp(log_weight * KERNEL_STEP + KERNEL_MID).T * (1.0 / (n * n))
    row = (cs_high[:, :], cs_low[:, :])
    cos = (cs_high[:, :n], cs_low[:, :n])
    sin = (cs_high[:, n:], cs_low[:, n:])
    u = halves(mul3(halves(grid), row))
    p = mul3(cos, u)
    q = mul3(sin, u)
    h_real = halves((p[:, :n] - q[:, n:]) * weight)
    h_imag = halves((p[:, n:] + q[:, :n]) * weight)
    g_real = halves(mul3(cos, h_real) + mul3(sin, h_imag))
    g_imag = halves(mul3(sin, h_real) - mul3(cos, h_imag))
    spread = mul3(g_real, cos) - mul3(g_imag, sin)
    level = level_of(jnp.max(jnp.abs(spread), axis=(0, 1), keepdims=True))
    codes = coded(spread, level).reshape(count // Y, Y // halved, depth, n)
    out_ref[:, half:] = to_16(jnp.broadcast_to(level[None, None], (count, 1, 2, lanes)))
    for upper in range(Y // halved):
        for side in range(halved):
            part = codes[:, upper, :, side * lanes : (side + 1) * lanes]
            start = (upper * halved + side) * (count // Y)
            part = part.reshape(count // Y, half, 2, lanes)
            out_ref[start : start + count // Y, :half] = to_16(part)


def return_kernel(back_ref, out_ref):
    block, half, _, lanes = back_ref.shape
    half = half - 1
    depth = 2 * half
    codes = from_16(back_ref[:, :half]).reshape(block, depth, lanes)
    codes = jnp.swapaxes(codes, 0, 1).reshape(depth, block // 2, 2, lanes)
    out_ref[:, : block // 2] = to_16(codes)
    level = from_16(back_ref[:, half, :1]).reshape(block, lanes)
    tail = to_lanes(level, 1)[:, None]
    out_ref[:, block // 2 :] = to_16(jnp.broadcast_to(tail, (depth, 1, 2, lanes)))


def exchange_kernel(spread_ref, chosen_ref, place_ref, out_ref):
    total, lanes = chosen_ref.shape[1:]
    potential = read_rows(spread_ref)
    orbs = lax.broadcasted_iota(jnp.int32, (total, lanes), 0).astype(jnp.float32)
    summed = jnp.zeros((total, 2 * lanes), jnp.float32)
    for c in range(2):
        contrib = potential * chosen_ref[1 - c].astype(jnp.float32)
        high, low = halves(contrib)
        select = [
            (orbs == place_ref[2 * j + c : 2 * j + c + 1]).astype(jnp.bfloat16)
            for j in range(total // lanes)
        ]
        summed += mul(jnp.concatenate(select, axis=1), jnp.concatenate([high, low], axis=1))
    write_rows(out_ref, -(summed[:, :lanes] + summed[:, lanes:]))


def home_kernel(home_ref, out_ref):
    count, rows, width = out_ref.shape
    values = read_rows(home_ref).reshape(Z, rows // Z, width // LANES, count, LANES)
    for upper in range(rows // Z):
        for side in range(width // LANES):
            part = jnp.swapaxes(values[:, upper, side], 0, 1)
            lanes = slice(side * LANES, (side + 1) * LANES)
            out_ref[:, upper * Z : (upper + 1) * Z, lanes] = part


def local(kernel, out, name, scalars=0):
    def call(*operands):
        specs = [pl.BlockSpec(memory_space=pltpu.SMEM)] * scalars
        specs += [pl.BlockSpec(memory_space=pltpu.VMEM)] * (len(operands) - scalars)
        return pl.pallas_call(kernel, out_shape=out, in_specs=specs, name=name)(*operands)

    return call


def message(n, pairs, dtype=jnp.int16):
    return jax.ShapeDtypeStruct((n, pairs, 2, LANES), dtype)


def swap(x, axis):
    return lax.all_to_all(x, axis, split_axis=0, concat_axis=0, tiled=True)


def on_device(orbitals, kernel, partner_owner, partner_local):
    orb_dev, rows_x, width_y = orbitals.shape
    tasks = partner_local.shape[0]
    peers = Z * Y
    total = peers * orb_dev
    block = Y * tasks
    sides = width_y // LANES
    here = jnp.stack([lax.axis_index("y"), lax.axis_index("fft") % 2])
    both = np.concatenate(tables(width_y), axis=1)
    high = both.astype(jnp.bfloat16)
    low = (both - high.astype(np.float32)).astype(jnp.bfloat16)
    shape = (Z, Y // sides, sides, orb_dev // 2 + 1, 2, LANES)
    packed = local(pack_kernel, jax.ShapeDtypeStruct(shape, jnp.bfloat16), "pack")(
        orbitals, partner_owner, partner_local
    )
    first = swap(packed.reshape(peers, *shape[3:]), ("z", "y"))
    outs = (
        message(Z, block // 2 + 1),
        jax.ShapeDtypeStruct((2, total, LANES), jnp.bfloat16),
        jax.ShapeDtypeStruct((2 * total // LANES, LANES), jnp.float32),
    )
    there, chosen, place = local(density_kernel, outs, "density")(first)
    there = swap(there, "z")
    there = local(onward_kernel, message(block, Z + 1), "onward", 1)(here, there, kernel)
    there = swap(there, ("y", "fft"))
    back = local(transform_kernel, message(block, Z // 2 + 1), "potential", 1)(
        here, there, jnp.asarray(high), jnp.asarray(low)
    )
    back = swap(back, ("y", "fft"))
    back = swap(local(return_kernel, message(Z, block // 2 + 1), "return")(back), "z")
    home = local(exchange_kernel, message(peers, orb_dev // 2 + 1), "exchange")(
        back, chosen, place
    )
    home = swap(home, ("z", "y"))
    result = jax.ShapeDtypeStruct(orbitals.shape, jnp.float32)
    return local(home_kernel, result, "home")(home)


def solution(mesh):
    devices = mesh.devices.reshape(Z, Y, mesh.devices.shape[1])
    fine = Mesh(devices, ("z", "y", "fft"))
    orb = ("z", "y")
    in_specs = (P(orb, "fft", None), P("fft", None), P(orb, None, None), P(orb, None))
    out_specs = P(orb, "fft", None)
    return jax.shard_map(
        on_device, mesh=fine, in_specs=in_specs, out_specs=out_specs, check_vma=False
    )
```

```python
import math

import jax
import jax.numpy as jnp
import numpy as np
from jax import lax
from jax.experimental import pallas as pl
from jax.experimental.pallas import tpu as pltpu
from jax.sharding import Mesh
from jax.sharding import PartitionSpec as P

Z, Y = 16, 4
LANES = 128
TOP = 32767.0
STEPS = 128.0
FLOOR = 1e-37
KERNEL_LOW, KERNEL_HIGH = 0.02, 2.0
KERNEL_MID = 0.5 * (math.log(KERNEL_HIGH) + math.log(KERNEL_LOW))
KERNEL_STEP = 0.5 * (math.log(KERNEL_HIGH) - math.log(KERNEL_LOW)) / TOP


def tables(length):
    series = np.arange(length, dtype=np.int64)
    angle = (series[:, None] * series[None, :] % length) * (2.0 * math.pi / length)
    return np.cos(angle).astype(np.float32), np.sin(angle).astype(np.float32)


def level_of(largest):
    return jnp.ceil(jnp.log(jnp.maximum(largest, FLOOR)) * (STEPS / math.log(2.0))) + 1.0


def coded(values, level):
    share = jnp.sqrt(jnp.abs(values) * jnp.exp(level * (-math.log(2.0) / STEPS)))
    share = jnp.round(jnp.minimum(share, 1.0) * TOP)
    return jnp.where(values < 0, -share, share)


def decoded(codes, level):
    share = codes * (1.0 / TOP)
    return share * jnp.abs(share) * jnp.exp(level * (math.log(2.0) / STEPS))


def to_16(codes):
    return codes.astype(jnp.int32).astype(jnp.int16)


def from_16(codes):
    return codes.astype(jnp.int32).astype(jnp.float32)


def halves(a):
    high = a.astype(jnp.bfloat16)
    low = (a - high.astype(jnp.float32)).astype(jnp.bfloat16)
    return high, low


def mul(a, b):
    return jnp.dot(a, b, preferred_element_type=jnp.float32)


def mul3(a, b):
    return mul(a[0], b[0]) + (mul(a[0], b[1]) + mul(a[1], b[0]))


def lane_of(shape):
    return lax.broadcasted_iota(jnp.int32, shape, len(shape) - 1)


def transform_kernel(here_ref, data_ref, cs_high, cs_low, out_ref):
    n = cs_high.shape[0]
    count, _, _, lanes = data_ref.shape
    depth = n * n // (count * lanes)
    half = depth // 2
    halved = n // lanes

    def assembled(blocks):
        blocks = blocks.reshape(Y // halved, halved, count // Y, depth, lanes)
        sides = [
            jnp.concatenate(
                [blocks[upper, side][:, None] for upper in range(Y // halved)], axis=1
            ).reshape(n, lanes)
            for side in range(halved)
        ]
        return jnp.concatenate(sides, axis=1)

    codes = from_16(data_ref[:, :half]).reshape(count, depth, lanes)
    tail = from_16(data_ref[:, 2 * half, :1])
    tail = jnp.broadcast_to(tail, (count, depth, lanes))
    row = lax.broadcasted_iota(jnp.int32, tail.shape, 1)
    tail = jnp.where(lane_of(tail.shape) == row, tail, 0.0)
    grid = assembled(decoded(codes, jnp.sum(tail, axis=2, keepdims=True)))
    log_weight = assembled(from_16(data_ref[:, half : 2 * half]).reshape(count, depth, lanes))
    weight = jnp.exp(log_weight * KERNEL_STEP + KERNEL_MID).T * (1.0 / (n * n))
    row = (cs_high[:, :], cs_low[:, :])
    cos = (cs_high[:, :n], cs_low[:, :n])
    sin = (cs_high[:, n:], cs_low[:, n:])
    u = halves(mul3(halves(grid), row))
    p = mul3(cos, u)
    q = mul3(sin, u)
    h_real = halves((p[:, :n] - q[:, n:]) * weight)
    h_imag = halves((p[:, n:] + q[:, :n]) * weight)
    g_real = halves(mul3(cos, h_real) + mul3(sin, h_imag))
    g_imag = halves(mul3(sin, h_real) - mul3(cos, h_imag))
    spread = mul3(g_real, cos) - mul3(g_imag, sin)
    level = level_of(jnp.max(jnp.abs(spread), axis=(0, 1), keepdims=True))
    codes = coded(spread, level).reshape(count // Y, Y // halved, depth, n)
    pair = jnp.full((2, lanes), here_ref[0] // 2, jnp.int32)
    side = lax.broadcasted_iota(jnp.int32, (2, lanes), 0)
    kept = (lane_of((2, lanes)) == pair) & (side == here_ref[0] % 2)
    tail = jnp.where(kept, level, 0.0)
    out_ref[:, half:] = to_16(jnp.broadcast_to(tail[None, None], (count, 1, 2, lanes)))
    for upper in range(Y // halved):
        for side in range(halved):
            part = codes[:, upper, :, side * lanes : (side + 1) * lanes]
            start = (upper * halved + side) * (count // Y)
            part = part.reshape(count // Y, half, 2, lanes)
            out_ref[start : start + count // Y, :half] = to_16(part)


def potential_of(data, here, n):
    count, pairs, _, lanes = data.shape
    both = np.concatenate(tables(n), axis=1)
    high = both.astype(jnp.bfloat16)
    low = (both - high.astype(np.float32)).astype(jnp.bfloat16)
    vmem = pl.BlockSpec(memory_space=pltpu.VMEM)
    return pl.pallas_call(
        transform_kernel,
        out_shape=jax.ShapeDtypeStruct((count, pairs // 2 + 1, 2, lanes), jnp.int16),
        in_specs=[pl.BlockSpec(memory_space=pltpu.SMEM), vmem, vmem, vmem],
        name="potential",
    )(here, data, jnp.asarray(high), jnp.asarray(low))


def swap(x, axis):
    return lax.all_to_all(x, axis, split_axis=0, concat_axis=0, tiled=True)


def message(codes, *tails):
    n, rows, lanes = codes.shape
    return jnp.concatenate([codes.reshape(n, rows // 2, 2, lanes), *tails], axis=1)


def codes_of(x):
    n, pairs, _, lanes = x.shape
    return x[:, : pairs - 1].reshape(n, (pairs - 1) * 2, lanes)


def tail_sum(x):
    return jnp.sum(x[:, -1].astype(jnp.int32), axis=0).astype(jnp.int16)


def block_level(values):
    return level_of(jnp.max(jnp.abs(values), axis=(1, 2), keepdims=True))


def on_device(orbitals, kernel, partner_owner, partner_local):
    orb_dev, rows_x, width_y = orbitals.shape
    tasks = partner_local.shape[0]
    peers = Z * Y
    total = peers * orb_dev
    block = Y * tasks
    sides = width_y // LANES
    own_z, own_y = lax.axis_index("z"), lax.axis_index("y")
    own_task = (own_y * tasks + lax.axis_index("fft")).reshape(1)
    cut = orbitals.reshape(orb_dev, Y // sides, Z, sides, LANES).transpose(2, 1, 3, 0, 4)
    names = (partner_owner[:, :, 0] * orb_dev + partner_local - 256).astype(jnp.bfloat16)
    names = jnp.pad(names.T, ((0, 0), (0, LANES - tasks)))
    names = jnp.broadcast_to(names[None, None], (peers, 1, 2, LANES))
    first = swap(message(cut.reshape(peers, orb_dev, LANES), names), ("z", "y"))
    table = codes_of(first).reshape(total, LANES)
    place = first[:, -1, :, :tasks].astype(jnp.int32).transpose(1, 0, 2).reshape(2 * total) + 256
    orbs = jnp.arange(total, dtype=jnp.int32)
    pick = (place[:, None] == orbs[None]).astype(jnp.bfloat16)
    chosen = mul(pick, table)
    left, right = chosen[:total], chosen[total:]
    density = (left * right).reshape(Z, block, LANES)
    level = block_level(density)
    tail = jnp.where(jnp.arange(LANES)[None, None, None] == own_z, level[:, None], 0.0)
    tail = jnp.broadcast_to(tail, (Z, 1, 2, LANES))
    there = message(to_16(coded(density, level)), to_16(tail))
    weight = to_16(jnp.round((jnp.log(kernel) - KERNEL_MID) * (1.0 / KERNEL_STEP)))
    weight = weight.reshape(Y // sides, Z, sides, LANES).transpose(0, 2, 1, 3)
    weight = lax.dynamic_index_in_dim(weight.reshape(Y, Z // 2, 2, LANES), own_y, 0)
    there, weight, own_task = lax.optimization_barrier((there, weight, own_task))
    there = swap(there, "z")
    tail = jnp.broadcast_to(tail_sum(there)[None, None], (block, 1, 2, LANES))
    weight = jnp.broadcast_to(weight, (block, Z // 2, 2, LANES))
    there = swap(message(codes_of(there).transpose(1, 0, 2), weight, tail), ("y", "fft"))
    back = swap(potential_of(there, own_task, width_y), ("y", "fft"))
    tail = jnp.broadcast_to(tail_sum(back)[None, None], (Z, 1, 2, LANES))
    spread = swap(message(codes_of(back).transpose(1, 0, 2), tail), "z")
    level = spread[:, -1, :, : block // 2].transpose(0, 2, 1).reshape(total, 1)
    potential = decoded(from_16(codes_of(spread)).reshape(total, LANES), from_16(level))
    contrib = jnp.concatenate([potential * right, potential * left], axis=0)
    select = (orbs[:, None] == place[None]).astype(jnp.bfloat16)
    high = lax.reduce_precision(contrib, 8, 7)
    low = (contrib - high).astype(jnp.bfloat16)
    summed = -(mul(select, high.astype(jnp.bfloat16)) + mul(select, low))
    summed = summed.reshape(peers, orb_dev, LANES)
    level = block_level(summed)
    tail = jnp.broadcast_to(to_16(level)[:, None], (peers, 1, 2, LANES))
    home = swap(message(to_16(coded(summed, level)), tail), ("z", "y"))
    result = decoded(from_16(codes_of(home)), from_16(home[:, -1, :1]))
    result = result.reshape(Z, Y // sides, sides, orb_dev, LANES).transpose(3, 1, 0, 2, 4)
    return result.reshape(orb_dev, rows_x, width_y)


def solution(mesh):
    devices = mesh.devices.reshape(Z, Y, mesh.devices.shape[1])
    fine = Mesh(devices, ("z", "y", "fft"))
    orb = ("z", "y")
    in_specs = (P(orb, "fft", None), P("fft", None), P(orb, None, None), P(orb, None))
    out_specs = P(orb, "fft", None)
    return jax.shard_map(
        on_device, mesh=fine, in_specs=in_specs, out_specs=out_specs, check_vma=False
    )
```

```python
import math

import jax
import jax.numpy as jnp
import numpy as np
from jax import lax
from jax.experimental import pallas as pl
from jax.experimental.pallas import tpu as pltpu
from jax.sharding import Mesh
from jax.sharding import PartitionSpec as P

Z, Y = 16, 4
LANES = 128
TOP = 32767.0
STEPS = 128.0
FLOOR = 1e-37
KERNEL_LOW, KERNEL_HIGH = 0.02, 2.0
KERNEL_MID = 0.5 * (math.log(KERNEL_HIGH) + math.log(KERNEL_LOW))
KERNEL_STEP = 0.5 * (math.log(KERNEL_HIGH) - math.log(KERNEL_LOW)) / TOP


def tables(length):
    series = np.arange(length, dtype=np.int64)
    angle = (series[:, None] * series[None, :] % length) * (2.0 * math.pi / length)
    return np.cos(angle).astype(np.float32), np.sin(angle).astype(np.float32)


def level_of(largest):
    return jnp.ceil(jnp.log(jnp.maximum(largest, FLOOR)) * (STEPS / math.log(2.0))) + 1.0


def coded(values, level):
    share = jnp.sqrt(jnp.abs(values) * jnp.exp(level * (-math.log(2.0) / STEPS)))
    share = jnp.round(jnp.minimum(share, 1.0) * TOP)
    return jnp.where(values < 0, -share, share)


def decoded(codes, level):
    share = codes * (1.0 / TOP)
    return share * jnp.abs(share) * jnp.exp(level * (math.log(2.0) / STEPS))


def to_16(codes):
    return codes.astype(jnp.int32).astype(jnp.int16)


def from_16(codes):
    return codes.astype(jnp.int32).astype(jnp.float32)


def halves(a):
    high = a.astype(jnp.bfloat16)
    low = (a - high.astype(jnp.float32)).astype(jnp.bfloat16)
    return high, low


def mul(a, b):
    return jnp.dot(a, b, preferred_element_type=jnp.float32)


def mul3(a, b):
    return mul(a[0], b[0]) + (mul(a[0], b[1]) + mul(a[1], b[0]))


def lane_of(shape):
    return lax.broadcasted_iota(jnp.int32, shape, len(shape) - 1)


def tail_sum(ref):
    return jnp.sum(ref[:, ref.shape[1] - 1].astype(jnp.int32), axis=0)


def turned(ref):
    n, pairs, _, lanes = ref.shape
    codes = ref[:, : pairs - 1].astype(jnp.int32).reshape(n, (pairs - 1) * 2, lanes)
    codes = jnp.swapaxes(codes, 0, 1).reshape((pairs - 1) * 2, n // 2, 2, lanes)
    return codes.astype(jnp.int16)


def block_level(values):
    return level_of(jnp.max(jnp.max(jnp.abs(values), axis=1, keepdims=True), axis=2, keepdims=True))


def pack_kernel(z_ref, y_ref, task_ref, orb_ref, owner_ref, local_ref, out_ref):
    count, rows, width = orb_ref.shape
    half = rows // Z
    orbs = orb_ref[...].astype(jnp.float32)
    for side in range(width // LANES):
        part = jnp.swapaxes(orbs[:, :, side * LANES : (side + 1) * LANES], 0, 1)
        for upper in range(half):
            piece = part[upper * Z : (upper + 1) * Z].reshape(Z, count // 2, 2, LANES)
            out_ref[:, upper, side, : count // 2] = piece.astype(jnp.bfloat16)
    names = (owner_ref[...] * count + local_ref[...] - 256).astype(jnp.float32)
    rest = jnp.zeros((2, LANES - names.shape[1]), jnp.float32)
    tail = jnp.concatenate([names, rest], axis=1).astype(jnp.bfloat16)
    shape = (Z, half, width // LANES, 1, 2, LANES)
    out_ref[:, :, :, count // 2 :] = jnp.broadcast_to(tail[None, None, None, None], shape)


def density_kernel(z_ref, first_ref, there_ref, chosen_ref, place_ref):
    peers, pairs, _, lanes = first_ref.shape
    pairs = pairs - 1
    total = peers * pairs * 2
    table = first_ref[:, :pairs].astype(jnp.float32).reshape(total, lanes).astype(jnp.bfloat16)
    tasks = total // peers
    group = lanes // tasks
    tails = first_ref[:, pairs].astype(jnp.float32).reshape(peers // group, group, 2, lanes)
    place = tails[:, 0]
    for s in range(1, group):
        place = place + pltpu.roll(tails[:, s], s * tasks, 2)
    place = place.reshape(2 * (peers // group), lanes) + 256.0
    place_ref[...] = place
    column = place.T
    orbs = lane_of((lanes, total)).astype(jnp.float32)
    sides = []
    for c in range(2):
        pick = [
            (orbs == column[:, 2 * j + c : 2 * j + c + 1]).astype(jnp.bfloat16)
            for j in range(total // lanes)
        ]
        sides.append(mul(jnp.concatenate(pick, axis=0), table))
        chosen_ref[c] = sides[c].astype(jnp.bfloat16)
    n, block = there_ref.shape[0], there_ref.shape[1] - 1
    density = (sides[0] * sides[1]).reshape(n, 2 * block, lanes)
    level = block_level(density)
    there_ref[:, :block] = to_16(coded(density, level).reshape(n, block, 2, lanes))
    shape = (n, 1, 2, lanes)
    tail = jnp.where(lane_of(shape) == z_ref[0], jnp.broadcast_to(level[:, None], shape), 0.0)
    there_ref[:, block:] = to_16(tail)


def onward_kernel(y_ref, there_ref, weight_ref, out_ref):
    depth, _, _, lanes = there_ref.shape
    block, half = out_ref.shape[0], depth // 2
    out_ref[:, :half] = turned(there_ref)
    tail = tail_sum(there_ref).astype(jnp.int16)
    out_ref[:, 2 * half :] = jnp.broadcast_to(tail[None, None], (block, 1, 2, lanes))
    own = jnp.zeros((depth, lanes), jnp.float32)
    halved = weight_ref.shape[1] // lanes
    for upper in range(weight_ref.shape[0] // depth):
        for side in range(halved):
            part = weight_ref[upper * depth : (upper + 1) * depth, side * lanes : (side + 1) * lanes]
            own = jnp.where(y_ref[0] == upper * halved + side, part, own)
    own = jnp.round((jnp.log(own) - KERNEL_MID) * (1.0 / KERNEL_STEP)).reshape(half, 2, lanes)
    out_ref[:, half : 2 * half] = jnp.broadcast_to(to_16(own)[None], (block, half, 2, lanes))


def transform_kernel(task_ref, data_ref, cs_high, cs_low, out_ref):
    n = cs_high.shape[0]
    count, _, _, lanes = data_ref.shape
    depth = n * n // (count * lanes)
    half = depth // 2
    halved = n // lanes

    def assembled(blocks):
        blocks = blocks.reshape(Y // halved, halved, count // Y, depth, lanes)
        sides = [
            jnp.concatenate(
                [blocks[upper, side][:, None] for upper in range(Y // halved)], axis=1
            ).reshape(n, lanes)
            for side in range(halved)
        ]
        return jnp.concatenate(sides, axis=1)

    codes = from_16(data_ref[:, :half]).reshape(count, depth, lanes)
    tail = from_16(data_ref[:, 2 * half, :1])
    tail = jnp.broadcast_to(tail, (count, depth, lanes))
    row = lax.broadcasted_iota(jnp.int32, tail.shape, 1)
    tail = jnp.where(lane_of(tail.shape) == row, tail, 0.0)
    grid = assembled(decoded(codes, jnp.sum(tail, axis=2, keepdims=True)))
    log_weight = assembled(from_16(data_ref[:, half : 2 * half]).reshape(count, depth, lanes))
    weight = jnp.exp(log_weight * KERNEL_STEP + KERNEL_MID).T * (1.0 / (n * n))
    row = (cs_high[:, :], cs_low[:, :])
    cos = (cs_high[:, :n], cs_low[:, :n])
    sin = (cs_high[:, n:], cs_low[:, n:])
    u = halves(mul3(halves(grid), row))
    p = mul3(cos, u)
    q = mul3(sin, u)
    h_real = halves((p[:, :n] - q[:, n:]) * weight)
    h_imag = halves((p[:, n:] + q[:, :n]) * weight)
    g_real = halves(mul3(cos, h_real) + mul3(sin, h_imag))
    g_imag = halves(mul3(sin, h_real) - mul3(cos, h_imag))
    spread = mul3(g_real, cos) - mul3(g_imag, sin)
    level = level_of(jnp.max(jnp.abs(spread), axis=(0, 1), keepdims=True))
    codes = coded(spread, level).reshape(count // Y, Y // halved, depth, n)
    pair = jnp.full((2, lanes), task_ref[0] // 2, jnp.int32)
    side = lax.broadcasted_iota(jnp.int32, (2, lanes), 0)
    kept = (lane_of((2, lanes)) == pair) & (side == task_ref[0] % 2)
    tail = jnp.where(kept, level, 0.0)
    out_ref[:, half:] = to_16(jnp.broadcast_to(tail[None, None], (count, 1, 2, lanes)))
    for upper in range(Y // halved):
        for side in range(halved):
            part = codes[:, upper, :, side * lanes : (side + 1) * lanes]
            start = (upper * halved + side) * (count // Y)
            part = part.reshape(count // Y, half, 2, lanes)
            out_ref[start : start + count // Y, :half] = to_16(part)


def return_kernel(back_ref, out_ref):
    half = out_ref.shape[1] - 1
    out_ref[:, :half] = turned(back_ref)
    tail = tail_sum(back_ref).astype(jnp.int16)
    out_ref[:, half:] = jnp.broadcast_to(tail[None, None], (out_ref.shape[0], 1, 2, tail.shape[1]))


def exchange_kernel(spread_ref, chosen_ref, place_ref, out_ref):
    total, lanes = chosen_ref.shape[1:]
    n, pairs = spread_ref.shape[0], spread_ref.shape[1] - 1
    tail = from_16(spread_ref[:, pairs])
    tail = jnp.broadcast_to(tail[:, None], (n, pairs, 2, lanes)).reshape(n, 2 * pairs, lanes)
    row = lax.broadcasted_iota(jnp.int32, tail.shape, 1)
    tail = jnp.where(lane_of(tail.shape) == row // 2, tail, 0.0).reshape(total, lanes)
    level = jnp.sum(tail, axis=1, keepdims=True)
    codes = from_16(spread_ref[:, :pairs]).reshape(total, lanes)
    potential = decoded(codes, level)
    orbs = lax.broadcasted_iota(jnp.int32, (total, lanes), 0).astype(jnp.float32)
    summed = jnp.zeros((total, 2 * lanes), jnp.float32)
    for c in range(2):
        contrib = potential * chosen_ref[1 - c].astype(jnp.float32)
        high, low = halves(contrib)
        select = [
            (orbs == place_ref[2 * j + c : 2 * j + c + 1]).astype(jnp.bfloat16)
            for j in range(total // lanes)
        ]
        summed += mul(jnp.concatenate(select, axis=1), jnp.concatenate([high, low], axis=1))
    peers, half = out_ref.shape[0], out_ref.shape[1] - 1
    summed = -(summed[:, :lanes] + summed[:, lanes:]).reshape(peers, 2 * half, lanes)
    level = block_level(summed)
    out_ref[:, :half] = to_16(coded(summed, level).reshape(peers, half, 2, lanes))
    out_ref[:, half:] = to_16(jnp.broadcast_to(level[:, None], (peers, 1, 2, lanes)))


def home_kernel(home_ref, out_ref):
    count, rows, width = out_ref.shape
    peers, half = home_ref.shape[0], home_ref.shape[1] - 1
    codes = from_16(home_ref[:, :half]).reshape(peers, 2 * half, LANES)
    values = decoded(codes, from_16(home_ref[:, half])[:, :1])
    values = values.reshape(Z, rows // Z, width // LANES, count, LANES)
    for upper in range(rows // Z):
        for side in range(width // LANES):
            part = jnp.swapaxes(values[:, upper, side], 0, 1)
            lanes = slice(side * LANES, (side + 1) * LANES)
            out_ref[:, upper * Z : (upper + 1) * Z, lanes] = part


def local(kernel, out, name, scalars=0):
    def call(*operands):
        specs = [pl.BlockSpec(memory_space=pltpu.SMEM)] * scalars
        specs += [pl.BlockSpec(memory_space=pltpu.VMEM)] * (len(operands) - scalars)
        params = pltpu.CompilerParams(vmem_limit_bytes=16 * 2**20)
        return pl.pallas_call(
            kernel, out_shape=out, in_specs=specs, compiler_params=params, name=name
        )(*operands)

    return call


def message(n, pairs, dtype=jnp.int16):
    return jax.ShapeDtypeStruct((n, pairs, 2, LANES), dtype)


def swap(x, axis):
    return lax.all_to_all(x, axis, split_axis=0, concat_axis=0, tiled=True)


def on_device(orbitals, kernel, partner_owner, partner_local):
    orb_dev, rows_x, width_y = orbitals.shape
    tasks = partner_local.shape[0]
    peers = Z * Y
    total = peers * orb_dev
    block = Y * tasks
    sides = width_y // LANES
    own_z, own_y = lax.axis_index("z").reshape(1), lax.axis_index("y").reshape(1)
    own_task = own_y * tasks + lax.axis_index("fft")
    both = np.concatenate(tables(width_y), axis=1)
    high = both.astype(jnp.bfloat16)
    low = (both - high.astype(np.float32)).astype(jnp.bfloat16)
    shape = (Z, Y // sides, sides, orb_dev // 2 + 1, 2, LANES)
    packed = local(pack_kernel, jax.ShapeDtypeStruct(shape, jnp.bfloat16), "pack", 3)(
        own_z, own_y, own_task, orbitals, partner_owner[:, :, 0].T, partner_local.T
    )
    first = swap(packed.reshape(peers, *shape[3:]), ("z", "y"))
    outs = (
        message(Z, block // 2 + 1),
        jax.ShapeDtypeStruct((2, total, LANES), jnp.bfloat16),
        jax.ShapeDtypeStruct((2 * total // LANES, LANES), jnp.float32),
    )
    there, chosen, place = local(density_kernel, outs, "density", 1)(own_z, first)
    there = swap(there, "z")
    there = local(onward_kernel, message(block, Z + 1), "onward", 1)(own_y, there, kernel)
    there = swap(there, ("y", "fft"))
    back = local(transform_kernel, message(block, Z // 2 + 1), "potential", 1)(
        own_task, there, jnp.asarray(high), jnp.asarray(low)
    )
    back = swap(back, ("y", "fft"))
    back = swap(local(return_kernel, message(Z, block // 2 + 1), "return")(back), "z")
    home = local(exchange_kernel, message(peers, orb_dev // 2 + 1), "exchange")(
        back, chosen, place
    )
    home = swap(home, ("z", "y"))
    result = jax.ShapeDtypeStruct(orbitals.shape, jnp.float32)
    return local(home_kernel, result, "home")(home)


def solution(mesh):
    devices = mesh.devices.reshape(Z, Y, mesh.devices.shape[1])
    fine = Mesh(devices, ("z", "y", "fft"))
    orb = ("z", "y")
    in_specs = (P(orb, "fft", None), P("fft", None), P(orb, None, None), P(orb, None))
    out_specs = P(orb, "fft", None)
    return jax.shard_map(
        on_device, mesh=fine, in_specs=in_specs, out_specs=out_specs, check_vma=False
    )
```

```python
import math

import jax
import jax.numpy as jnp
import numpy as np
from jax import lax
from jax.experimental import pallas as pl
from jax.experimental.pallas import tpu as pltpu
from jax.sharding import Mesh
from jax.sharding import PartitionSpec as P

Z, Y = 16, 4
LANES = 128
TOP = 32767.0
STEPS = 128.0
FLOOR = 1e-37
KERNEL_LOW, KERNEL_HIGH = 0.02, 2.0
KERNEL_MID = 0.5 * (math.log(KERNEL_HIGH) + math.log(KERNEL_LOW))
KERNEL_STEP = 0.5 * (math.log(KERNEL_HIGH) - math.log(KERNEL_LOW)) / TOP


def tables(length):
    series = np.arange(length, dtype=np.int64)
    angle = (series[:, None] * series[None, :] % length) * (2.0 * math.pi / length)
    return np.cos(angle).astype(np.float32), np.sin(angle).astype(np.float32)


def level_of(largest):
    return jnp.ceil(jnp.log(jnp.maximum(largest, FLOOR)) * (STEPS / math.log(2.0))) + 1.0


def coded(values, level):
    share = jnp.sqrt(jnp.abs(values) * jnp.exp(level * (-math.log(2.0) / STEPS)))
    share = jnp.round(jnp.minimum(share, 1.0) * TOP)
    return jnp.where(values < 0, -share, share)


def decoded(codes, level):
    share = codes * (1.0 / TOP)
    return share * jnp.abs(share) * jnp.exp(level * (math.log(2.0) / STEPS))


def to_16(codes):
    return codes.astype(jnp.int32).astype(jnp.int16)


def from_16(codes):
    return codes.astype(jnp.int32).astype(jnp.float32)


def halves(a):
    high = a.astype(jnp.bfloat16)
    low = (a - high.astype(jnp.float32)).astype(jnp.bfloat16)
    return high, low


def mul(a, b):
    return jnp.dot(a, b, preferred_element_type=jnp.float32)


def mul3(a, b):
    return mul(a[0], b[0]) + (mul(a[0], b[1]) + mul(a[1], b[0]))


def lane_of(shape):
    return lax.broadcasted_iota(jnp.int32, shape, len(shape) - 1)


def tail_sum(ref):
    return jnp.sum(ref[:, ref.shape[1] - 1].astype(jnp.int32), axis=0)


def turned(ref):
    n, pairs, _, lanes = ref.shape
    codes = ref[:, : pairs - 1].astype(jnp.int32).reshape(n, (pairs - 1) * 2, lanes)
    codes = jnp.swapaxes(codes, 0, 1).reshape((pairs - 1) * 2, n // 2, 2, lanes)
    return codes.astype(jnp.int16)


def block_level(values):
    return level_of(jnp.max(jnp.max(jnp.abs(values), axis=1, keepdims=True), axis=2, keepdims=True))


def pack_kernel(z_ref, y_ref, task_ref, orb_hbm, owner_hbm, local_hbm, out_ref, *scratch):
    orb_ref, owner_ref, local_ref, sems = scratch
    loads = [
        pltpu.make_async_copy(source, here, sems.at[i])
        for i, (source, here) in enumerate(
            ((owner_hbm, owner_ref), (local_hbm, local_ref), (orb_hbm, orb_ref))
        )
    ]
    for load in loads:
        load.start()
    for load in loads:
        load.wait()
    count, rows, width = orb_ref.shape
    half = rows // Z
    orbs = orb_ref[...].astype(jnp.float32)
    for side in range(width // LANES):
        part = jnp.swapaxes(orbs[:, :, side * LANES : (side + 1) * LANES], 0, 1)
        for upper in range(half):
            piece = part[upper * Z : (upper + 1) * Z].reshape(Z, count // 2, 2, LANES)
            out_ref[:, upper, side, : count // 2] = piece.astype(jnp.bfloat16)
    names = (owner_ref[...] * count + local_ref[...] - 256).astype(jnp.float32)
    rest = jnp.zeros((2, LANES - names.shape[1]), jnp.float32)
    tail = jnp.concatenate([names, rest], axis=1).astype(jnp.bfloat16)
    shape = (Z, half, width // LANES, 1, 2, LANES)
    out_ref[:, :, :, count // 2 :] = jnp.broadcast_to(tail[None, None, None, None], shape)


def density_kernel(z_ref, first_ref, there_ref, chosen_ref, place_ref):
    peers, pairs, _, lanes = first_ref.shape
    pairs = pairs - 1
    total = peers * pairs * 2
    table = first_ref[:, :pairs].astype(jnp.float32).reshape(total, lanes).astype(jnp.bfloat16)
    tasks = total // peers
    group = lanes // tasks
    tails = first_ref[:, pairs].astype(jnp.float32).reshape(peers // group, group, 2, lanes)
    place = tails[:, 0]
    for s in range(1, group):
        place = place + pltpu.roll(tails[:, s], s * tasks, 2)
    place = place.reshape(2 * (peers // group), lanes)
    place_ref[...] = place
    column = place.T
    orbs = lane_of((lanes, total)).astype(jnp.float32) - 256.0
    sides = []
    for c in range(2):
        pick = [
            (orbs == column[:, 2 * j + c : 2 * j + c + 1]).astype(jnp.bfloat16)
            for j in range(total // lanes)
        ]
        sides.append(mul(jnp.concatenate(pick, axis=0), table))
        chosen_ref[c] = sides[c].astype(jnp.bfloat16)
    n, block = there_ref.shape[0], there_ref.shape[1] - 1
    density = (sides[0] * sides[1]).reshape(n, 2 * block, lanes)
    level = block_level(density)
    there_ref[:, :block] = to_16(coded(density, level).reshape(n, block, 2, lanes))
    shape = (n, 1, 2, lanes)
    tail = jnp.where(lane_of(shape) == z_ref[0], jnp.broadcast_to(level[:, None], shape), 0.0)
    there_ref[:, block:] = to_16(tail)


def onward_kernel(y_ref, there_ref, weight_ref, out_ref):
    depth, _, _, lanes = there_ref.shape
    block, half = out_ref.shape[0], depth // 2
    out_ref[:, :half] = turned(there_ref)
    tail = tail_sum(there_ref).astype(jnp.int16)
    out_ref[:, 2 * half :] = jnp.broadcast_to(tail[None, None], (block, 1, 2, lanes))
    own = jnp.zeros((depth, lanes), jnp.float32)
    halved = weight_ref.shape[1] // lanes
    for upper in range(weight_ref.shape[0] // depth):
        for side in range(halved):
            part = weight_ref[upper * depth : (upper + 1) * depth, side * lanes : (side + 1) * lanes]
            own = jnp.where(y_ref[0] == upper * halved + side, part, own)
    own = jnp.round((jnp.log(own) - KERNEL_MID) * (1.0 / KERNEL_STEP)).reshape(half, 2, lanes)
    out_ref[:, half : 2 * half] = jnp.broadcast_to(to_16(own)[None], (block, half, 2, lanes))


def transform_kernel(task_ref, data_ref, cs_high, cs_low, out_ref):
    n = cs_high.shape[0]
    count, _, _, lanes = data_ref.shape
    depth = n * n // (count * lanes)
    half = depth // 2
    halved = n // lanes

    def assembled(blocks):
        blocks = blocks.reshape(Y // halved, halved, count // Y, depth, lanes)
        sides = [
            jnp.concatenate(
                [blocks[upper, side][:, None] for upper in range(Y // halved)], axis=1
            ).reshape(n, lanes)
            for side in range(halved)
        ]
        return jnp.concatenate(sides, axis=1)

    codes = from_16(data_ref[:, :half]).reshape(count, depth, lanes)
    tail = from_16(data_ref[:, 2 * half, :1])
    tail = jnp.broadcast_to(tail, (count, depth, lanes))
    row = lax.broadcasted_iota(jnp.int32, tail.shape, 1)
    tail = jnp.where(lane_of(tail.shape) == row, tail, 0.0)
    grid = assembled(decoded(codes, jnp.sum(tail, axis=2, keepdims=True)))
    log_weight = assembled(from_16(data_ref[:, half : 2 * half]).reshape(count, depth, lanes))
    weight = jnp.exp(log_weight * KERNEL_STEP + KERNEL_MID).T * (1.0 / (n * n))
    row = (cs_high[:, :], cs_low[:, :])
    cos = (cs_high[:, :n], cs_low[:, :n])
    sin = (cs_high[:, n:], cs_low[:, n:])
    u = halves(mul3(halves(grid), row))
    p = mul3(cos, u)
    q = mul3(sin, u)
    h_real = halves((p[:, :n] - q[:, n:]) * weight)
    h_imag = halves((p[:, n:] + q[:, :n]) * weight)
    g_real = halves(mul3(cos, h_real) + mul3(sin, h_imag))
    g_imag = halves(mul3(sin, h_real) - mul3(cos, h_imag))
    spread = mul3(g_real, cos) - mul3(g_imag, sin)
    level = level_of(jnp.max(jnp.abs(spread), axis=(0, 1), keepdims=True))
    codes = coded(spread, level).reshape(count // Y, Y // halved, depth, n)
    pair = jnp.full((2, lanes), task_ref[0] // 2, jnp.int32)
    side = lax.broadcasted_iota(jnp.int32, (2, lanes), 0)
    kept = (lane_of((2, lanes)) == pair) & (side == task_ref[0] % 2)
    tail = jnp.where(kept, level, 0.0)
    out_ref[:, half:] = to_16(jnp.broadcast_to(tail[None, None], (count, 1, 2, lanes)))
    for upper in range(Y // halved):
        for side in range(halved):
            part = codes[:, upper, :, side * lanes : (side + 1) * lanes]
            start = (upper * halved + side) * (count // Y)
            part = part.reshape(count // Y, half, 2, lanes)
            out_ref[start : start + count // Y, :half] = to_16(part)


def return_kernel(back_ref, out_ref):
    half = out_ref.shape[1] - 1
    out_ref[:, :half] = turned(back_ref)
    tail = tail_sum(back_ref).astype(jnp.int16)
    out_ref[:, half:] = jnp.broadcast_to(tail[None, None], (out_ref.shape[0], 1, 2, tail.shape[1]))


def exchange_kernel(spread_ref, chosen_ref, place_ref, out_ref):
    total, lanes = chosen_ref.shape[1:]
    n, pairs = spread_ref.shape[0], spread_ref.shape[1] - 1
    tail = from_16(spread_ref[:, pairs])
    tail = jnp.broadcast_to(tail[:, None], (n, pairs, 2, lanes)).reshape(n, 2 * pairs, lanes)
    row = lax.broadcasted_iota(jnp.int32, tail.shape, 1)
    tail = jnp.where(lane_of(tail.shape) == row // 2, tail, 0.0).reshape(total, lanes)
    level = jnp.sum(tail, axis=1, keepdims=True)
    codes = from_16(spread_ref[:, :pairs]).reshape(total, lanes)
    potential = decoded(codes, level)
    orbs = lax.broadcasted_iota(jnp.int32, (total, lanes), 0).astype(jnp.float32) - 256.0
    orbs = orbs.astype(jnp.bfloat16)
    one, zero = jnp.ones((), jnp.bfloat16), jnp.zeros((), jnp.bfloat16)
    place = place_ref[...].astype(jnp.bfloat16)
    summed = jnp.zeros((total, 2 * lanes), jnp.float32)
    for c in range(2):
        contrib = potential * chosen_ref[1 - c].astype(jnp.float32)
        high, low = halves(contrib)
        select = [
            jnp.where(orbs == place[2 * j + c : 2 * j + c + 1], one, zero)
            for j in range(total // lanes)
        ]
        summed += mul(jnp.concatenate(select, axis=1), jnp.concatenate([high, low], axis=1))
    peers, half = out_ref.shape[0], out_ref.shape[1] - 1
    summed = -(summed[:, :lanes] + summed[:, lanes:]).reshape(peers, 2 * half, lanes)
    level = block_level(summed)
    out_ref[:, :half] = to_16(coded(summed, level).reshape(peers, half, 2, lanes))
    out_ref[:, half:] = to_16(jnp.broadcast_to(level[:, None], (peers, 1, 2, lanes)))


def home_kernel(home_ref, out_hbm, out_ref, sems):
    count, rows, width = out_ref.shape
    peers, half = home_ref.shape[0], home_ref.shape[1] - 1
    codes = from_16(home_ref[:, :half]).reshape(peers, 2 * half, LANES)
    values = decoded(codes, from_16(home_ref[:, half])[:, :1])
    values = values.reshape(Z, rows // Z, width // LANES, count, LANES)
    stores = []
    for upper in range(rows // Z):
        half = pl.ds(upper * Z, Z)
        for side in range(width // LANES):
            part = jnp.swapaxes(values[:, upper, side], 0, 1)
            out_ref[:, half, side * LANES : (side + 1) * LANES] = part
        stores.append(
            pltpu.make_async_copy(out_ref.at[:, half], out_hbm.at[:, half], sems.at[upper])
        )
        stores[upper].start()
    for store in stores:
        store.wait()


def local(kernel, out, name, scalars=0, arrays=pltpu.VMEM, **more):
    def call(*operands):
        specs = [pl.BlockSpec(memory_space=pltpu.SMEM)] * scalars
        specs += [pl.BlockSpec(memory_space=arrays)] * (len(operands) - scalars)
        params = pltpu.CompilerParams(vmem_limit_bytes=16 * 2**20)
        return pl.pallas_call(
            kernel, out_shape=out, in_specs=specs, compiler_params=params, name=name, **more
        )(*operands)

    return call


def message(n, pairs, dtype=jnp.int16):
    return jax.ShapeDtypeStruct((n, pairs, 2, LANES), dtype)


def swap(x, axis):
    return lax.all_to_all(x, axis, split_axis=0, concat_axis=0, tiled=True)


def on_device(orbitals, kernel, partner_owner, partner_local):
    orb_dev, rows_x, width_y = orbitals.shape
    tasks = partner_local.shape[0]
    peers = Z * Y
    total = peers * orb_dev
    block = Y * tasks
    sides = width_y // LANES
    own_z, own_y = lax.axis_index("z").reshape(1), lax.axis_index("y").reshape(1)
    own_task = own_y * tasks + lax.axis_index("fft")
    both = np.concatenate(tables(width_y), axis=1)
    high = both.astype(jnp.bfloat16)
    low = (both - high.astype(np.float32)).astype(jnp.bfloat16)
    shape = (Z, Y // sides, sides, orb_dev // 2 + 1, 2, LANES)
    names = pltpu.VMEM((2, tasks), jnp.int32)
    scratch = [pltpu.VMEM(orbitals.shape, orbitals.dtype), names, names]
    scratch.append(pltpu.SemaphoreType.DMA((3,)))
    packed = jax.ShapeDtypeStruct(shape, jnp.bfloat16)
    packed = local(pack_kernel, packed, "pack", 3, pltpu.HBM, scratch_shapes=scratch)(
        own_z, own_y, own_task, orbitals, partner_owner[:, :, 0].T, partner_local.T
    )
    first = swap(packed.reshape(peers, *shape[3:]), ("z", "y"))
    outs = (
        message(Z, block // 2 + 1),
        jax.ShapeDtypeStruct((2, total, LANES), jnp.bfloat16),
        jax.ShapeDtypeStruct((2 * total // LANES, LANES), jnp.float32),
    )
    there, chosen, place = local(density_kernel, outs, "density", 1)(own_z, first)
    there = swap(there, "z")
    there = local(onward_kernel, message(block, Z + 1), "onward", 1)(own_y, there, kernel)
    there = swap(there, ("y", "fft"))
    back = local(transform_kernel, message(block, Z // 2 + 1), "potential", 1)(
        own_task, there, jnp.asarray(high), jnp.asarray(low)
    )
    back = swap(back, ("y", "fft"))
    back = swap(local(return_kernel, message(Z, block // 2 + 1), "return")(back), "z")
    home = local(exchange_kernel, message(peers, orb_dev // 2 + 1), "exchange")(
        back, chosen, place
    )
    home = swap(home, ("z", "y"))
    result = jax.ShapeDtypeStruct(orbitals.shape, jnp.float32)
    scratch = [pltpu.VMEM(orbitals.shape, jnp.float32), pltpu.SemaphoreType.DMA((rows_x // Z,))]
    spec = pl.BlockSpec(memory_space=pltpu.HBM)
    return local(home_kernel, result, "home", out_specs=spec, scratch_shapes=scratch)(home)


def solution(mesh):
    devices = mesh.devices.reshape(Z, Y, mesh.devices.shape[1])
    fine = Mesh(devices, ("z", "y", "fft"))
    orb = ("z", "y")
    in_specs = (P(orb, "fft", None), P("fft", None), P(orb, None, None), P(orb, None))
    out_specs = P(orb, "fft", None)
    return jax.shard_map(
        on_device, mesh=fine, in_specs=in_specs, out_specs=out_specs, check_vma=False
    )
```

```python
import math

import jax
import jax.numpy as jnp
import numpy as np
from jax import lax
from jax.experimental import pallas as pl
from jax.experimental.pallas import tpu as pltpu
from jax.sharding import Mesh
from jax.sharding import PartitionSpec as P

Z, Y = 16, 4
LANES = 128
TOP = 32767.0
STEPS = 128.0
FLOOR = 1e-37
KERNEL_LOW, KERNEL_HIGH = 0.02, 2.0
KERNEL_MID = 0.5 * (math.log(KERNEL_HIGH) + math.log(KERNEL_LOW))
KERNEL_STEP = 0.5 * (math.log(KERNEL_HIGH) - math.log(KERNEL_LOW)) / TOP


def tables(length):
    series = np.arange(length, dtype=np.int64)
    angle = (series[:, None] * series[None, :] % length) * (2.0 * math.pi / length)
    return np.cos(angle).astype(np.float32), np.sin(angle).astype(np.float32)


def level_of(largest):
    return jnp.ceil(jnp.log(jnp.maximum(largest, FLOOR)) * (STEPS / math.log(2.0))) + 1.0


def coded(values, level):
    share = jnp.sqrt(jnp.abs(values) * jnp.exp(level * (-math.log(2.0) / STEPS)))
    share = jnp.round(jnp.minimum(share, 1.0) * TOP)
    return jnp.where(values < 0, -share, share)


def decoded(codes, level):
    share = codes * (1.0 / TOP)
    return share * jnp.abs(share) * jnp.exp(level * (math.log(2.0) / STEPS))


def to_16(codes):
    return codes.astype(jnp.int32).astype(jnp.int16)


def from_16(codes):
    return codes.astype(jnp.int32).astype(jnp.float32)


def halves(a):
    high = a.astype(jnp.bfloat16)
    low = (a - high.astype(jnp.float32)).astype(jnp.bfloat16)
    return high, low


def mul(a, b):
    return jnp.dot(a, b, preferred_element_type=jnp.float32)


def mul3(a, b):
    return mul(a[0], b[0]) + (mul(a[0], b[1]) + mul(a[1], b[0]))


def lane_of(shape):
    return lax.broadcasted_iota(jnp.int32, shape, len(shape) - 1)


def tail_sum(ref):
    return jnp.sum(ref[:, ref.shape[1] - 1].astype(jnp.int32), axis=0)


def turned(ref):
    n, pairs, _, lanes = ref.shape
    codes = ref[:, : pairs - 1].astype(jnp.int32).reshape(n, (pairs - 1) * 2, lanes)
    codes = jnp.swapaxes(codes, 0, 1).reshape((pairs - 1) * 2, n // 2, 2, lanes)
    return codes.astype(jnp.int16)


def block_level(values):
    return level_of(jnp.max(jnp.max(jnp.abs(values), axis=1, keepdims=True), axis=2, keepdims=True))


def pack_kernel(z_ref, y_ref, task_ref, orb_hbm, owner_hbm, local_hbm, out_ref, *scratch):
    orb_ref, owner_ref, local_ref, sems = scratch
    loads = [
        pltpu.make_async_copy(source, here, sems.at[i])
        for i, (source, here) in enumerate(
            ((owner_hbm, owner_ref), (local_hbm, local_ref), (orb_hbm, orb_ref))
        )
    ]
    for load in loads:
        load.start()
    for load in loads:
        load.wait()
    count, rows, width = orb_ref.shape
    half = rows // Z
    orbs = orb_ref[...].astype(jnp.float32)
    for side in range(width // LANES):
        part = jnp.swapaxes(orbs[:, :, side * LANES : (side + 1) * LANES], 0, 1)
        for upper in range(half):
            piece = part[upper * Z : (upper + 1) * Z].reshape(Z, count // 2, 2, LANES)
            out_ref[:, upper, side, : count // 2] = piece.astype(jnp.bfloat16)
    names = (owner_ref[...] * count + local_ref[...] - 256).astype(jnp.float32)
    rest = jnp.zeros((2, LANES - names.shape[1]), jnp.float32)
    tail = jnp.concatenate([names, rest], axis=1).astype(jnp.bfloat16)
    shape = (Z, half, width // LANES, 1, 2, LANES)
    out_ref[:, :, :, count // 2 :] = jnp.broadcast_to(tail[None, None, None, None], shape)


def density_kernel(z_ref, first_ref, there_ref, chosen_ref, place_ref):
    peers, pairs, _, lanes = first_ref.shape
    pairs = pairs - 1
    total = peers * pairs * 2
    table = first_ref[:, :pairs].astype(jnp.float32).reshape(total, lanes).astype(jnp.bfloat16)
    tasks = total // peers
    group = lanes // tasks
    tails = first_ref[:, pairs].astype(jnp.float32).reshape(peers // group, group, 2, lanes)
    place = tails[:, 0]
    for s in range(1, group):
        place = place + pltpu.roll(tails[:, s], s * tasks, 2)
    place = place.reshape(2 * (peers // group), lanes) + 256.0
    place_ref[...] = place
    column = place.T
    orbs = lane_of((lanes, total)).astype(jnp.float32)
    sides = []
    for c in range(2):
        pick = [
            (orbs == column[:, 2 * j + c : 2 * j + c + 1]).astype(jnp.bfloat16)
            for j in range(total // lanes)
        ]
        sides.append(mul(jnp.concatenate(pick, axis=0), table))
        chosen_ref[c] = sides[c].astype(jnp.bfloat16)
    n, block = there_ref.shape[0], there_ref.shape[1] - 1
    density = (sides[0] * sides[1]).reshape(n, 2 * block, lanes)
    level = block_level(density)
    there_ref[:, :block] = to_16(coded(density, level).reshape(n, block, 2, lanes))
    shape = (n, 1, 2, lanes)
    tail = jnp.where(lane_of(shape) == z_ref[0], jnp.broadcast_to(level[:, None], shape), 0.0)
    there_ref[:, block:] = to_16(tail)


def onward_kernel(y_ref, there_ref, weight_ref, out_ref):
    depth, _, _, lanes = there_ref.shape
    block, half = out_ref.shape[0], depth // 2
    out_ref[:, :half] = turned(there_ref)
    tail = tail_sum(there_ref).astype(jnp.int16)
    out_ref[:, 2 * half :] = jnp.broadcast_to(tail[None, None], (block, 1, 2, lanes))
    own = jnp.zeros((depth, lanes), jnp.float32)
    halved = weight_ref.shape[1] // lanes
    for upper in range(weight_ref.shape[0] // depth):
        for side in range(halved):
            part = weight_ref[upper * depth : (upper + 1) * depth, side * lanes : (side + 1) * lanes]
            own = jnp.where(y_ref[0] == upper * halved + side, part, own)
    own = jnp.round((jnp.log(own) - KERNEL_MID) * (1.0 / KERNEL_STEP)).reshape(half, 2, lanes)
    out_ref[:, half : 2 * half] = jnp.broadcast_to(to_16(own)[None], (block, half, 2, lanes))


def transform_kernel(task_ref, data_ref, cs_high, cs_low, out_ref):
    n = cs_high.shape[0]
    count, _, _, lanes = data_ref.shape
    depth = n * n // (count * lanes)
    half = depth // 2
    halved = n // lanes

    def assembled(blocks):
        blocks = blocks.reshape(Y // halved, halved, count // Y, depth, lanes)
        sides = [
            jnp.concatenate(
                [blocks[upper, side][:, None] for upper in range(Y // halved)], axis=1
            ).reshape(n, lanes)
            for side in range(halved)
        ]
        return jnp.concatenate(sides, axis=1)

    codes = from_16(data_ref[:, :half]).reshape(count, depth, lanes)
    tail = from_16(data_ref[:, 2 * half, :1])
    tail = jnp.broadcast_to(tail, (count, depth, lanes))
    row = lax.broadcasted_iota(jnp.int32, tail.shape, 1)
    tail = jnp.where(lane_of(tail.shape) == row, tail, 0.0)
    grid = assembled(decoded(codes, jnp.sum(tail, axis=2, keepdims=True)))
    log_weight = assembled(from_16(data_ref[:, half : 2 * half]).reshape(count, depth, lanes))
    weight = jnp.exp(log_weight * KERNEL_STEP + KERNEL_MID).T * (1.0 / (n * n))
    row = (cs_high[:, :], cs_low[:, :])
    cos = (cs_high[:, :n], cs_low[:, :n])
    sin = (cs_high[:, n:], cs_low[:, n:])
    u = halves(mul3(halves(grid), row))
    p = mul3(cos, u)
    q = mul3(sin, u)
    h_real = halves((p[:, :n] - q[:, n:]) * weight)
    h_imag = halves((p[:, n:] + q[:, :n]) * weight)
    g_real = halves(mul3(cos, h_real) + mul3(sin, h_imag))
    g_imag = halves(mul3(sin, h_real) - mul3(cos, h_imag))
    spread = mul3(g_real, cos) - mul3(g_imag, sin)
    level = level_of(jnp.max(jnp.abs(spread), axis=(0, 1), keepdims=True))
    codes = coded(spread, level).reshape(count // Y, Y // halved, depth, n)
    pair = jnp.full((2, lanes), task_ref[0] // 2, jnp.int32)
    side = lax.broadcasted_iota(jnp.int32, (2, lanes), 0)
    kept = (lane_of((2, lanes)) == pair) & (side == task_ref[0] % 2)
    tail = jnp.where(kept, level, 0.0)
    out_ref[:, half:] = to_16(jnp.broadcast_to(tail[None, None], (count, 1, 2, lanes)))
    for upper in range(Y // halved):
        for side in range(halved):
            part = codes[:, upper, :, side * lanes : (side + 1) * lanes]
            start = (upper * halved + side) * (count // Y)
            part = part.reshape(count // Y, half, 2, lanes)
            out_ref[start : start + count // Y, :half] = to_16(part)


def return_kernel(back_ref, out_ref):
    half = out_ref.shape[1] - 1
    out_ref[:, :half] = turned(back_ref)
    tail = tail_sum(back_ref).astype(jnp.int16)
    out_ref[:, half:] = jnp.broadcast_to(tail[None, None], (out_ref.shape[0], 1, 2, tail.shape[1]))


def exchange_kernel(spread_ref, chosen_ref, place_ref, out_ref):
    total, lanes = chosen_ref.shape[1:]
    n, pairs = spread_ref.shape[0], spread_ref.shape[1] - 1
    tail = from_16(spread_ref[:, pairs])
    tail = jnp.broadcast_to(tail[:, None], (n, pairs, 2, lanes)).reshape(n, 2 * pairs, lanes)
    row = lax.broadcasted_iota(jnp.int32, tail.shape, 1)
    tail = jnp.where(lane_of(tail.shape) == row // 2, tail, 0.0).reshape(total, lanes)
    level = jnp.sum(tail, axis=1, keepdims=True)
    codes = from_16(spread_ref[:, :pairs]).reshape(total, lanes)
    potential = decoded(codes, level)
    orbs = lax.broadcasted_iota(jnp.int32, (total, lanes), 0).astype(jnp.float32)
    summed = jnp.zeros((total, 2 * lanes), jnp.float32)
    for c in range(2):
        contrib = potential * chosen_ref[1 - c].astype(jnp.float32)
        high, low = halves(contrib)
        select = [
            (orbs == place_ref[2 * j + c : 2 * j + c + 1]).astype(jnp.bfloat16)
            for j in range(total // lanes)
        ]
        summed += mul(jnp.concatenate(select, axis=1), jnp.concatenate([high, low], axis=1))
    peers, half = out_ref.shape[0], out_ref.shape[1] - 1
    summed = -(summed[:, :lanes] + summed[:, lanes:]).reshape(peers, 2 * half, lanes)
    level = block_level(summed)
    out_ref[:, :half] = to_16(coded(summed, level).reshape(peers, half, 2, lanes))
    out_ref[:, half:] = to_16(jnp.broadcast_to(level[:, None], (peers, 1, 2, lanes)))


def home_kernel(home_ref, out_hbm, out_ref, sems):
    count, rows, width = out_ref.shape
    peers, half = home_ref.shape[0], home_ref.shape[1] - 1
    codes = from_16(home_ref[:, :half]).reshape(peers, 2 * half, LANES)
    values = decoded(codes, from_16(home_ref[:, half])[:, :1])
    values = values.reshape(Z, rows // Z, width // LANES, count, LANES)
    stores = []
    for upper in range(rows // Z):
        half = pl.ds(upper * Z, Z)
        for side in range(width // LANES):
            part = jnp.swapaxes(values[:, upper, side], 0, 1)
            out_ref[:, half, side * LANES : (side + 1) * LANES] = part
        stores.append(
            pltpu.make_async_copy(out_ref.at[:, half], out_hbm.at[:, half], sems.at[upper])
        )
        stores[upper].start()
    for store in stores:
        store.wait()


def local(kernel, out, name, scalars=0, arrays=pltpu.VMEM, **more):
    def call(*operands):
        specs = [pl.BlockSpec(memory_space=pltpu.SMEM)] * scalars
        specs += [pl.BlockSpec(memory_space=arrays)] * (len(operands) - scalars)
        params = pltpu.CompilerParams(vmem_limit_bytes=16 * 2**20)
        return pl.pallas_call(
            kernel, out_shape=out, in_specs=specs, compiler_params=params, name=name, **more
        )(*operands)

    return call


def message(n, pairs, dtype=jnp.int16):
    return jax.ShapeDtypeStruct((n, pairs, 2, LANES), dtype)


def swap(x, axis):
    return lax.all_to_all(x, axis, split_axis=0, concat_axis=0, tiled=True)


def on_device(orbitals, kernel, partner_owner, partner_local):
    orb_dev, rows_x, width_y = orbitals.shape
    tasks = partner_local.shape[0]
    peers = Z * Y
    total = peers * orb_dev
    block = Y * tasks
    sides = width_y // LANES
    own_z, own_y = lax.axis_index("z").reshape(1), lax.axis_index("y").reshape(1)
    own_task = own_y * tasks + lax.axis_index("fft")
    both = np.concatenate(tables(width_y), axis=1)
    high = both.astype(jnp.bfloat16)
    low = (both - high.astype(np.float32)).astype(jnp.bfloat16)
    shape = (Z, Y // sides, sides, orb_dev // 2 + 1, 2, LANES)
    far = (orbitals, partner_owner[:, :, 0].T, partner_local.T)
    far = [pltpu.with_memory_space_constraint(x, pltpu.HBM) for x in far]
    names = pltpu.VMEM((2, tasks), jnp.int32)
    scratch = [pltpu.VMEM(orbitals.shape, orbitals.dtype), names, names]
    scratch.append(pltpu.SemaphoreType.DMA((3,)))
    packed = jax.ShapeDtypeStruct(shape, jnp.bfloat16)
    packed = local(pack_kernel, packed, "pack", 3, pltpu.HBM, scratch_shapes=scratch)(
        own_z, own_y, own_task, *far
    )
    first = swap(packed.reshape(peers, *shape[3:]), ("z", "y"))
    outs = (
        message(Z, block // 2 + 1),
        jax.ShapeDtypeStruct((2, total, LANES), jnp.bfloat16),
        jax.ShapeDtypeStruct((2 * total // LANES, LANES), jnp.float32),
    )
    there, chosen, place = local(density_kernel, outs, "density", 1)(own_z, first)
    there = swap(there, "z")
    there = local(onward_kernel, message(block, Z + 1), "onward", 1)(own_y, there, kernel)
    there = swap(there, ("y", "fft"))
    back = local(transform_kernel, message(block, Z // 2 + 1), "potential", 1)(
        own_task, there, jnp.asarray(high), jnp.asarray(low)
    )
    back = swap(back, ("y", "fft"))
    back = swap(local(return_kernel, message(Z, block // 2 + 1), "return")(back), "z")
    home = local(exchange_kernel, message(peers, orb_dev // 2 + 1), "exchange")(
        back, chosen, place
    )
    home = swap(home, ("z", "y"))
    result = jax.ShapeDtypeStruct(orbitals.shape, jnp.float32)
    scratch = [pltpu.VMEM(orbitals.shape, jnp.float32), pltpu.SemaphoreType.DMA((rows_x // Z,))]
    spec = pl.BlockSpec(memory_space=pltpu.HBM)
    return local(home_kernel, result, "home", out_specs=spec, scratch_shapes=scratch)(home)


def solution(mesh):
    devices = mesh.devices.reshape(Z, Y, mesh.devices.shape[1])
    fine = Mesh(devices, ("z", "y", "fft"))
    orb = ("z", "y")
    in_specs = (P(orb, "fft", None), P("fft", None), P(orb, None, None), P(orb, None))
    out_specs = P(orb, "fft", None)
    return jax.shard_map(
        on_device, mesh=fine, in_specs=in_specs, out_specs=out_specs, check_vma=False
    )
```

```python
import math

import jax
import jax.numpy as jnp
import numpy as np
from jax import lax
from jax.experimental import pallas as pl
from jax.experimental.pallas import tpu as pltpu
from jax.sharding import Mesh
from jax.sharding import PartitionSpec as P

Z, Y = 16, 4
LANES = 128
TOP = 32767.0
STEPS = 128.0
FLOOR = 1e-37
KERNEL_LOW, KERNEL_HIGH = 0.02, 2.0
KERNEL_MID = 0.5 * (math.log(KERNEL_HIGH) + math.log(KERNEL_LOW))
KERNEL_STEP = 0.5 * (math.log(KERNEL_HIGH) - math.log(KERNEL_LOW)) / TOP


def tables(length):
    series = np.arange(length, dtype=np.int64)
    angle = (series[:, None] * series[None, :] % length) * (2.0 * math.pi / length)
    return np.cos(angle).astype(np.float32), np.sin(angle).astype(np.float32)


def level_of(largest):
    return jnp.ceil(jnp.log(jnp.maximum(largest, FLOOR)) * (STEPS / math.log(2.0))) + 1.0


def coded(values, level):
    share = jnp.sqrt(jnp.abs(values) * jnp.exp(level * (-math.log(2.0) / STEPS)))
    share = jnp.round(jnp.minimum(share, 1.0) * TOP)
    return jnp.where(values < 0, -share, share)


def decoded(codes, level):
    share = codes * (1.0 / TOP)
    return share * jnp.abs(share) * jnp.exp(level * (math.log(2.0) / STEPS))


def to_16(codes):
    return codes.astype(jnp.int32).astype(jnp.int16)


def from_16(codes):
    return codes.astype(jnp.int32).astype(jnp.float32)


def halves(a):
    high = a.astype(jnp.bfloat16)
    low = (a - high.astype(jnp.float32)).astype(jnp.bfloat16)
    return high, low


def mul(a, b):
    return jnp.dot(a, b, preferred_element_type=jnp.float32)


def mul3(a, b):
    return mul(a[0], b[0]) + (mul(a[0], b[1]) + mul(a[1], b[0]))


def lane_of(shape):
    return lax.broadcasted_iota(jnp.int32, shape, len(shape) - 1)


def tail_sum(ref):
    return jnp.sum(ref[:, ref.shape[1] - 1].astype(jnp.int32), axis=0)


def turned(ref):
    n, pairs, _, lanes = ref.shape
    codes = ref[:, : pairs - 1].astype(jnp.int32).reshape(n, (pairs - 1) * 2, lanes)
    codes = jnp.swapaxes(codes, 0, 1).reshape((pairs - 1) * 2, n // 2, 2, lanes)
    return codes.astype(jnp.int16)


def block_level(values):
    return level_of(jnp.max(jnp.max(jnp.abs(values), axis=1, keepdims=True), axis=2, keepdims=True))


def pack_kernel(z_ref, y_ref, task_ref, orb_hbm, owner_hbm, local_hbm, out_ref, *scratch):
    orb_ref, owner_ref, local_ref, sems = scratch
    loads = [
        pltpu.make_async_copy(source, here, sems.at[i])
        for i, (source, here) in enumerate(
            ((owner_hbm, owner_ref), (local_hbm, local_ref), (orb_hbm, orb_ref))
        )
    ]
    for load in loads:
        load.start()
    for load in loads:
        load.wait()
    count, rows, width = orb_ref.shape
    half = rows // Z
    orbs = orb_ref[...].astype(jnp.float32)
    for side in range(width // LANES):
        part = jnp.swapaxes(orbs[:, :, side * LANES : (side + 1) * LANES], 0, 1)
        for upper in range(half):
            piece = part[upper * Z : (upper + 1) * Z].reshape(Z, count // 2, 2, LANES)
            out_ref[:, upper, side, : count // 2] = piece.astype(jnp.bfloat16)
    names = (owner_ref[...] * count + local_ref[...] - 256).astype(jnp.float32)
    rest = jnp.zeros((2, LANES - names.shape[1]), jnp.float32)
    tail = jnp.concatenate([names, rest], axis=1).astype(jnp.bfloat16)
    shape = (Z, half, width // LANES, 1, 2, LANES)
    out_ref[:, :, :, count // 2 :] = jnp.broadcast_to(tail[None, None, None, None], shape)


def density_kernel(z_ref, first_ref, there_ref, chosen_ref, place_ref):
    peers, pairs, _, lanes = first_ref.shape
    pairs = pairs - 1
    total = peers * pairs * 2
    table = first_ref[:, :pairs].reshape(total, lanes)
    tasks = total // peers
    group = lanes // tasks
    tails = first_ref[:, pairs].astype(jnp.float32).reshape(peers // group, group, 2, lanes)
    place = tails[:, 0]
    for s in range(1, group):
        place = place + pltpu.roll(tails[:, s], s * tasks, 2)
    place = place.reshape(2 * (peers // group), lanes) + 256.0
    place_ref[...] = place
    column = place.T
    orbs = lane_of((lanes, total)).astype(jnp.float32)
    sides = []
    for c in range(2):
        pick = [
            (orbs == column[:, 2 * j + c : 2 * j + c + 1]).astype(jnp.bfloat16)
            for j in range(total // lanes)
        ]
        sides.append(mul(jnp.concatenate(pick, axis=0), table))
        chosen_ref[c] = sides[c].astype(jnp.bfloat16)
    n, block = there_ref.shape[0], there_ref.shape[1] - 1
    density = (sides[0] * sides[1]).reshape(n, 2 * block, lanes)
    level = block_level(density)
    there_ref[:, :block] = to_16(coded(density, level)).reshape(n, block, 2, lanes)
    shape = (n, 1, 2, lanes)
    tail = jnp.where(lane_of(shape) == z_ref[0], jnp.broadcast_to(level[:, None], shape), 0.0)
    there_ref[:, block:] = to_16(tail)


def onward_kernel(y_ref, there_ref, weight_ref, out_ref):
    depth, _, _, lanes = there_ref.shape
    block, half = out_ref.shape[0], depth // 2
    out_ref[:, :half] = turned(there_ref)
    tail = tail_sum(there_ref).astype(jnp.int16)
    out_ref[:, 2 * half :] = jnp.broadcast_to(tail[None, None], (block, 1, 2, lanes))
    own = jnp.zeros((depth, lanes), jnp.float32)
    halved = weight_ref.shape[1] // lanes
    for upper in range(weight_ref.shape[0] // depth):
        for side in range(halved):
            part = weight_ref[upper * depth : (upper + 1) * depth, side * lanes : (side + 1) * lanes]
            own = jnp.where(y_ref[0] == upper * halved + side, part, own)
    own = jnp.round((jnp.log(own) - KERNEL_MID) * (1.0 / KERNEL_STEP)).reshape(half, 2, lanes)
    out_ref[:, half : 2 * half] = jnp.broadcast_to(to_16(own)[None], (block, half, 2, lanes))


def transform_kernel(task_ref, data_ref, cs_high, cs_low, out_ref):
    n = cs_high.shape[0]
    count, _, _, lanes = data_ref.shape
    depth = n * n // (count * lanes)
    half = depth // 2
    halved = n // lanes

    def assembled(blocks):
        blocks = blocks.reshape(Y // halved, halved, count // Y, depth, lanes)
        sides = [
            jnp.concatenate(
                [blocks[upper, side][:, None] for upper in range(Y // halved)], axis=1
            ).reshape(n, lanes)
            for side in range(halved)
        ]
        return jnp.concatenate(sides, axis=1)

    codes = from_16(data_ref[:, :half].reshape(count, depth, lanes))
    tail = from_16(data_ref[:, 2 * half, :1])
    tail = jnp.broadcast_to(tail, (count, depth, lanes))
    row = lax.broadcasted_iota(jnp.int32, tail.shape, 1)
    tail = jnp.where(lane_of(tail.shape) == row, tail, 0.0)
    grid = assembled(decoded(codes, jnp.sum(tail, axis=2, keepdims=True)))
    log_weight = assembled(from_16(data_ref[:, half : 2 * half].reshape(count, depth, lanes)))
    weight = jnp.exp(log_weight * KERNEL_STEP + KERNEL_MID).T * (1.0 / (n * n))
    row = (cs_high[:, :], cs_low[:, :])
    cos = (cs_high[:, :n], cs_low[:, :n])
    sin = (cs_high[:, n:], cs_low[:, n:])
    u = halves(mul3(halves(grid), row))
    p = mul3(cos, u)
    q = mul3(sin, u)
    h_real = halves((p[:, :n] - q[:, n:]) * weight)
    h_imag = halves((p[:, n:] + q[:, :n]) * weight)
    g_real = halves(mul3(cos, h_real) + mul3(sin, h_imag))
    g_imag = halves(mul3(sin, h_real) - mul3(cos, h_imag))
    spread = mul3(g_real, cos) - mul3(g_imag, sin)
    level = level_of(jnp.max(jnp.abs(spread), axis=(0, 1), keepdims=True))
    codes = coded(spread, level).reshape(count // Y, Y // halved, depth, n)
    pair = jnp.full((2, lanes), task_ref[0] // 2, jnp.int32)
    side = lax.broadcasted_iota(jnp.int32, (2, lanes), 0)
    kept = (lane_of((2, lanes)) == pair) & (side == task_ref[0] % 2)
    tail = jnp.where(kept, level, 0.0)
    out_ref[:, half:] = to_16(jnp.broadcast_to(tail[None, None], (count, 1, 2, lanes)))
    for upper in range(Y // halved):
        for side in range(halved):
            part = codes[:, upper, :, side * lanes : (side + 1) * lanes]
            start = (upper * halved + side) * (count // Y)
            part = to_16(part).reshape(count // Y, half, 2, lanes)
            out_ref[start : start + count // Y, :half] = part


def return_kernel(back_ref, out_ref):
    half = out_ref.shape[1] - 1
    out_ref[:, :half] = turned(back_ref)
    tail = tail_sum(back_ref).astype(jnp.int16)
    out_ref[:, half:] = jnp.broadcast_to(tail[None, None], (out_ref.shape[0], 1, 2, tail.shape[1]))


def exchange_kernel(spread_ref, chosen_ref, place_ref, out_ref):
    total, lanes = chosen_ref.shape[1:]
    n, pairs = spread_ref.shape[0], spread_ref.shape[1] - 1
    tail = from_16(spread_ref[:, pairs])
    tail = jnp.broadcast_to(tail[:, None], (n, pairs, 2, lanes)).reshape(n, 2 * pairs, lanes)
    row = lax.broadcasted_iota(jnp.int32, tail.shape, 1)
    tail = jnp.where(lane_of(tail.shape) == row // 2, tail, 0.0).reshape(total, lanes)
    level = jnp.sum(tail, axis=1, keepdims=True)
    codes = from_16(spread_ref[:, :pairs].reshape(total, lanes))
    potential = decoded(codes, level)
    orbs = lax.broadcasted_iota(jnp.int32, (total, lanes), 0).astype(jnp.float32)
    summed = jnp.zeros((total, 2 * lanes), jnp.float32)
    for c in range(2):
        contrib = potential * chosen_ref[1 - c].astype(jnp.float32)
        high, low = halves(contrib)
        select = [
            (orbs == place_ref[2 * j + c : 2 * j + c + 1]).astype(jnp.bfloat16)
            for j in range(total // lanes)
        ]
        summed += mul(jnp.concatenate(select, axis=1), jnp.concatenate([high, low], axis=1))
    peers, half = out_ref.shape[0], out_ref.shape[1] - 1
    summed = -(summed[:, :lanes] + summed[:, lanes:]).reshape(peers, 2 * half, lanes)
    level = block_level(summed)
    out_ref[:, :half] = to_16(coded(summed, level)).reshape(peers, half, 2, lanes)
    out_ref[:, half:] = to_16(jnp.broadcast_to(level[:, None], (peers, 1, 2, lanes)))


def home_kernel(home_ref, out_hbm, out_ref, sems):
    count, rows, width = out_ref.shape
    peers, half = home_ref.shape[0], home_ref.shape[1] - 1
    codes = from_16(home_ref[:, :half].reshape(peers, 2 * half, LANES))
    values = decoded(codes, from_16(home_ref[:, half])[:, :1])
    values = values.reshape(Z, rows // Z, width // LANES, count, LANES)
    stores = []
    for upper in range(rows // Z):
        half = pl.ds(upper * Z, Z)
        for side in range(width // LANES):
            part = jnp.swapaxes(values[:, upper, side], 0, 1)
            out_ref[:, half, side * LANES : (side + 1) * LANES] = part
        stores.append(
            pltpu.make_async_copy(out_ref.at[:, half], out_hbm.at[:, half], sems.at[upper])
        )
        stores[upper].start()
    for store in stores:
        store.wait()


def local(kernel, out, name, scalars=0, arrays=pltpu.VMEM, **more):
    def call(*operands):
        specs = [pl.BlockSpec(memory_space=pltpu.SMEM)] * scalars
        specs += [pl.BlockSpec(memory_space=arrays)] * (len(operands) - scalars)
        params = pltpu.CompilerParams(vmem_limit_bytes=16 * 2**20)
        return pl.pallas_call(
            kernel, out_shape=out, in_specs=specs, compiler_params=params, name=name, **more
        )(*operands)

    return call


def message(n, pairs, dtype=jnp.int16):
    return jax.ShapeDtypeStruct((n, pairs, 2, LANES), dtype)


def swap(x, axis):
    return lax.all_to_all(x, axis, split_axis=0, concat_axis=0, tiled=True)


def on_device(orbitals, kernel, partner_owner, partner_local):
    orb_dev, rows_x, width_y = orbitals.shape
    tasks = partner_local.shape[0]
    peers = Z * Y
    total = peers * orb_dev
    block = Y * tasks
    sides = width_y // LANES
    own_z, own_y = lax.axis_index("z").reshape(1), lax.axis_index("y").reshape(1)
    own_task = own_y * tasks + lax.axis_index("fft")
    both = np.concatenate(tables(width_y), axis=1)
    high = both.astype(jnp.bfloat16)
    low = (both - high.astype(np.float32)).astype(jnp.bfloat16)
    shape = (Z, Y // sides, sides, orb_dev // 2 + 1, 2, LANES)
    far = (orbitals, partner_owner[:, :, 0].T, partner_local.T)
    far = [pltpu.with_memory_space_constraint(x, pltpu.HBM) for x in far]
    names = pltpu.VMEM((2, tasks), jnp.int32)
    scratch = [pltpu.VMEM(orbitals.shape, orbitals.dtype), names, names]
    scratch.append(pltpu.SemaphoreType.DMA((3,)))
    packed = jax.ShapeDtypeStruct(shape, jnp.bfloat16)
    packed = local(pack_kernel, packed, "pack", 3, pltpu.HBM, scratch_shapes=scratch)(
        own_z, own_y, own_task, *far
    )
    first = swap(packed.reshape(peers, *shape[3:]), ("z", "y"))
    outs = (
        message(Z, block // 2 + 1),
        jax.ShapeDtypeStruct((2, total, LANES), jnp.bfloat16),
        jax.ShapeDtypeStruct((2 * total // LANES, LANES), jnp.float32),
    )
    there, chosen, place = local(density_kernel, outs, "density", 1)(own_z, first)
    there = swap(there, "z")
    there = local(onward_kernel, message(block, Z + 1), "onward", 1)(own_y, there, kernel)
    there = swap(there, ("y", "fft"))
    back = local(transform_kernel, message(block, Z // 2 + 1), "potential", 1)(
        own_task, there, jnp.asarray(high), jnp.asarray(low)
    )
    back = swap(back, ("y", "fft"))
    back = swap(local(return_kernel, message(Z, block // 2 + 1), "return")(back), "z")
    home = local(exchange_kernel, message(peers, orb_dev // 2 + 1), "exchange")(
        back, chosen, place
    )
    home = swap(home, ("z", "y"))
    result = jax.ShapeDtypeStruct(orbitals.shape, jnp.float32)
    scratch = [pltpu.VMEM(orbitals.shape, jnp.float32), pltpu.SemaphoreType.DMA((rows_x // Z,))]
    spec = pl.BlockSpec(memory_space=pltpu.HBM)
    return local(home_kernel, result, "home", out_specs=spec, scratch_shapes=scratch)(home)


def solution(mesh):
    devices = mesh.devices.reshape(Z, Y, mesh.devices.shape[1])
    fine = Mesh(devices, ("z", "y", "fft"))
    orb = ("z", "y")
    in_specs = (P(orb, "fft", None), P("fft", None), P(orb, None, None), P(orb, None))
    out_specs = P(orb, "fft", None)
    return jax.shard_map(
        on_device, mesh=fine, in_specs=in_specs, out_specs=out_specs, check_vma=False
    )
```

```python
import math

import jax
import jax.numpy as jnp
import numpy as np
from jax import lax
from jax.experimental import pallas as pl
from jax.experimental.pallas import tpu as pltpu
from jax.sharding import Mesh
from jax.sharding import PartitionSpec as P

Z, Y = 16, 4
LANES = 128
TOP = 32767.0
STEPS = 128.0
FLOOR = 1e-37
KERNEL_LOW, KERNEL_HIGH = 0.02, 2.0
KERNEL_MID = 0.5 * (math.log(KERNEL_HIGH) + math.log(KERNEL_LOW))
KERNEL_STEP = 0.5 * (math.log(KERNEL_HIGH) - math.log(KERNEL_LOW)) / TOP


def tables(length):
    series = np.arange(length, dtype=np.int64)
    angle = (series[:, None] * series[None, :] % length) * (2.0 * math.pi / length)
    return np.cos(angle).astype(np.float32), np.sin(angle).astype(np.float32)


def level_of(largest):
    return jnp.ceil(jnp.log(jnp.maximum(largest, FLOOR)) * (STEPS / math.log(2.0))) + 1.0


def coded(values, level):
    share = jnp.sqrt(jnp.abs(values) * jnp.exp(level * (-math.log(2.0) / STEPS)))
    share = jnp.round(jnp.minimum(share, 1.0) * TOP)
    return jnp.where(values < 0, -share, share)


def decoded(codes, level):
    share = codes * (1.0 / TOP)
    return share * jnp.abs(share) * jnp.exp(level * (math.log(2.0) / STEPS))


def to_16(codes):
    return codes.astype(jnp.int32).astype(jnp.int16)


def from_16(codes):
    return codes.astype(jnp.int32).astype(jnp.float32)


def halves(a):
    high = a.astype(jnp.bfloat16)
    low = (a - high.astype(jnp.float32)).astype(jnp.bfloat16)
    return high, low


def mul(a, b):
    return jnp.dot(a, b, preferred_element_type=jnp.float32)


def mul3(a, b):
    return mul(a[0], b[0]) + (mul(a[0], b[1]) + mul(a[1], b[0]))


def lane_of(shape):
    return lax.broadcasted_iota(jnp.int32, shape, len(shape) - 1)


def tail_sum(ref):
    return jnp.sum(ref[:, ref.shape[1] - 1].astype(jnp.int32), axis=0)


def turned(ref):
    n, pairs, _, lanes = ref.shape
    codes = ref[:, : pairs - 1].astype(jnp.int32).reshape(n, (pairs - 1) * 2, lanes)
    codes = jnp.swapaxes(codes, 0, 1).reshape((pairs - 1) * 2, n // 2, 2, lanes)
    return codes.astype(jnp.int16)


def block_level(values):
    return level_of(jnp.max(jnp.max(jnp.abs(values), axis=1, keepdims=True), axis=2, keepdims=True))


def pack_kernel(z_ref, y_ref, task_ref, orb_hbm, owner_hbm, local_hbm, out_ref, *scratch):
    orb_ref, owner_ref, local_ref, sems = scratch
    count, rows, width = orb_ref.shape
    half = rows // Z
    loads = [
        pltpu.make_async_copy(orb_hbm.at[:, pl.ds(i * Z, Z)], orb_ref.at[:, pl.ds(i * Z, Z)], sems.at[i])
        for i in range(half)
    ]
    loads.append(pltpu.make_async_copy(owner_hbm, owner_ref, sems.at[half]))
    loads.append(pltpu.make_async_copy(local_hbm, local_ref, sems.at[half + 1]))
    for load in loads:
        load.start()
    for upper in range(half):
        loads[upper].wait()
        orbs = orb_ref[:, upper * Z : (upper + 1) * Z].astype(jnp.float32)
        for side in range(width // LANES):
            part = jnp.swapaxes(orbs[:, :, side * LANES : (side + 1) * LANES], 0, 1)
            piece = part.reshape(Z, count // 2, 2, LANES)
            out_ref[:, upper, side, : count // 2] = piece.astype(jnp.bfloat16)
    loads[half].wait()
    loads[half + 1].wait()
    names = (owner_ref[...] * count + local_ref[...] - 256).astype(jnp.float32)
    rest = jnp.zeros((2, LANES - names.shape[1]), jnp.float32)
    tail = jnp.concatenate([names, rest], axis=1).astype(jnp.bfloat16)
    shape = (Z, half, width // LANES, 1, 2, LANES)
    out_ref[:, :, :, count // 2 :] = jnp.broadcast_to(tail[None, None, None, None], shape)


def density_kernel(z_ref, first_ref, there_ref, chosen_ref, place_ref):
    peers, pairs, _, lanes = first_ref.shape
    pairs = pairs - 1
    total = peers * pairs * 2
    table = first_ref[:, :pairs].reshape(total, lanes)
    tasks = total // peers
    group = lanes // tasks
    tails = first_ref[:, pairs].astype(jnp.float32).reshape(peers // group, group, 2, lanes)
    place = tails[:, 0]
    for s in range(1, group):
        place = place + pltpu.roll(tails[:, s], s * tasks, 2)
    place = place.reshape(2 * (peers // group), lanes) + 256.0
    place_ref[...] = place
    column = place.T
    orbs = lane_of((lanes, total)).astype(jnp.float32)
    sides = []
    for c in range(2):
        pick = [
            (orbs == column[:, 2 * j + c : 2 * j + c + 1]).astype(jnp.bfloat16)
            for j in range(total // lanes)
        ]
        sides.append(mul(jnp.concatenate(pick, axis=0), table))
        chosen_ref[c] = sides[c].astype(jnp.bfloat16)
    n, block = there_ref.shape[0], there_ref.shape[1] - 1
    density = (sides[0] * sides[1]).reshape(n, 2 * block, lanes)
    level = block_level(density)
    there_ref[:, :block] = to_16(coded(density, level)).reshape(n, block, 2, lanes)
    shape = (n, 1, 2, lanes)
    tail = jnp.where(lane_of(shape) == z_ref[0], jnp.broadcast_to(level[:, None], shape), 0.0)
    there_ref[:, block:] = to_16(tail)


def onward_kernel(y_ref, there_ref, weight_ref, out_ref):
    depth, _, _, lanes = there_ref.shape
    block, half = out_ref.shape[0], depth // 2
    out_ref[:, :half] = turned(there_ref)
    tail = tail_sum(there_ref).astype(jnp.int16)
    out_ref[:, 2 * half :] = jnp.broadcast_to(tail[None, None], (block, 1, 2, lanes))
    own = jnp.zeros((depth, lanes), jnp.float32)
    halved = weight_ref.shape[1] // lanes
    for upper in range(weight_ref.shape[0] // depth):
        for side in range(halved):
            part = weight_ref[upper * depth : (upper + 1) * depth, side * lanes : (side + 1) * lanes]
            own = jnp.where(y_ref[0] == upper * halved + side, part, own)
    own = jnp.round((jnp.log(own) - KERNEL_MID) * (1.0 / KERNEL_STEP)).reshape(half, 2, lanes)
    out_ref[:, half : 2 * half] = jnp.broadcast_to(to_16(own)[None], (block, half, 2, lanes))


def transform_kernel(task_ref, data_ref, cs_high, cs_low, out_ref):
    n = cs_high.shape[0]
    count, _, _, lanes = data_ref.shape
    depth = n * n // (count * lanes)
    half = depth // 2
    halved = n // lanes

    def assembled(blocks):
        blocks = blocks.reshape(Y // halved, halved, count // Y, depth, lanes)
        sides = [
            jnp.concatenate(
                [blocks[upper, side][:, None] for upper in range(Y // halved)], axis=1
            ).reshape(n, lanes)
            for side in range(halved)
        ]
        return jnp.concatenate(sides, axis=1)

    codes = from_16(data_ref[:, :half].reshape(count, depth, lanes))
    tail = from_16(data_ref[:, 2 * half, :1])
    tail = jnp.broadcast_to(tail, (count, depth, lanes))
    row = lax.broadcasted_iota(jnp.int32, tail.shape, 1)
    tail = jnp.where(lane_of(tail.shape) == row, tail, 0.0)
    grid = assembled(decoded(codes, jnp.sum(tail, axis=2, keepdims=True)))
    log_weight = assembled(from_16(data_ref[:, half : 2 * half].reshape(count, depth, lanes)))
    weight = jnp.exp(log_weight * KERNEL_STEP + KERNEL_MID).T * (1.0 / (n * n))
    row = (cs_high[:, :], cs_low[:, :])
    cos = (cs_high[:, :n], cs_low[:, :n])
    sin = (cs_high[:, n:], cs_low[:, n:])
    u = halves(mul3(halves(grid), row))
    p = mul3(cos, u)
    q = mul3(sin, u)
    h_real = halves((p[:, :n] - q[:, n:]) * weight)
    h_imag = halves((p[:, n:] + q[:, :n]) * weight)
    g_real = halves(mul3(cos, h_real) + mul3(sin, h_imag))
    g_imag = halves(mul3(sin, h_real) - mul3(cos, h_imag))
    spread = mul3(g_real, cos) - mul3(g_imag, sin)
    level = level_of(jnp.max(jnp.abs(spread), axis=(0, 1), keepdims=True))
    codes = coded(spread, level).reshape(count // Y, Y // halved, depth, n)
    pair = jnp.full((2, lanes), task_ref[0] // 2, jnp.int32)
    side = lax.broadcasted_iota(jnp.int32, (2, lanes), 0)
    kept = (lane_of((2, lanes)) == pair) & (side == task_ref[0] % 2)
    tail = jnp.where(kept, level, 0.0)
    out_ref[:, half:] = to_16(jnp.broadcast_to(tail[None, None], (count, 1, 2, lanes)))
    for upper in range(Y // halved):
        for side in range(halved):
            part = codes[:, upper, :, side * lanes : (side + 1) * lanes]
            start = (upper * halved + side) * (count // Y)
            part = to_16(part).reshape(count // Y, half, 2, lanes)
            out_ref[start : start + count // Y, :half] = part


def return_kernel(back_ref, out_ref):
    half = out_ref.shape[1] - 1
    out_ref[:, :half] = turned(back_ref)
    tail = tail_sum(back_ref).astype(jnp.int16)
    out_ref[:, half:] = jnp.broadcast_to(tail[None, None], (out_ref.shape[0], 1, 2, tail.shape[1]))


def exchange_kernel(spread_ref, chosen_ref, place_ref, out_ref):
    total, lanes = chosen_ref.shape[1:]
    n, pairs = spread_ref.shape[0], spread_ref.shape[1] - 1
    tail = from_16(spread_ref[:, pairs])
    tail = jnp.broadcast_to(tail[:, None], (n, pairs, 2, lanes)).reshape(n, 2 * pairs, lanes)
    row = lax.broadcasted_iota(jnp.int32, tail.shape, 1)
    tail = jnp.where(lane_of(tail.shape) == row // 2, tail, 0.0).reshape(total, lanes)
    level = jnp.sum(tail, axis=1, keepdims=True)
    codes = from_16(spread_ref[:, :pairs].reshape(total, lanes))
    potential = decoded(codes, level)
    orbs = lax.broadcasted_iota(jnp.int32, (total, lanes), 0).astype(jnp.float32)
    summed = jnp.zeros((total, 2 * lanes), jnp.float32)
    for c in range(2):
        contrib = potential * chosen_ref[1 - c].astype(jnp.float32)
        high, low = halves(contrib)
        select = [
            (orbs == place_ref[2 * j + c : 2 * j + c + 1]).astype(jnp.bfloat16)
            for j in range(total // lanes)
        ]
        summed += mul(jnp.concatenate(select, axis=1), jnp.concatenate([high, low], axis=1))
    peers, half = out_ref.shape[0], out_ref.shape[1] - 1
    summed = -(summed[:, :lanes] + summed[:, lanes:]).reshape(peers, 2 * half, lanes)
    level = block_level(summed)
    out_ref[:, :half] = to_16(coded(summed, level)).reshape(peers, half, 2, lanes)
    out_ref[:, half:] = to_16(jnp.broadcast_to(level[:, None], (peers, 1, 2, lanes)))


def home_kernel(home_ref, out_hbm, out_ref, sems):
    count, rows, width = out_ref.shape
    peers, half = home_ref.shape[0], home_ref.shape[1] - 1
    codes = from_16(home_ref[:, :half].reshape(peers, 2 * half, LANES))
    values = decoded(codes, from_16(home_ref[:, half])[:, :1])
    values = values.reshape(Z, rows // Z, width // LANES, count, LANES)
    stores = []
    for upper in range(rows // Z):
        half = pl.ds(upper * Z, Z)
        for side in range(width // LANES):
            part = jnp.swapaxes(values[:, upper, side], 0, 1)
            out_ref[:, half, side * LANES : (side + 1) * LANES] = part
        stores.append(
            pltpu.make_async_copy(out_ref.at[:, half], out_hbm.at[:, half], sems.at[upper])
        )
        stores[upper].start()
    for store in stores:
        store.wait()


def local(kernel, out, name, scalars=0, arrays=pltpu.VMEM, **more):
    def call(*operands):
        specs = [pl.BlockSpec(memory_space=pltpu.SMEM)] * scalars
        specs += [pl.BlockSpec(memory_space=arrays)] * (len(operands) - scalars)
        params = pltpu.CompilerParams(vmem_limit_bytes=16 * 2**20)
        return pl.pallas_call(
            kernel, out_shape=out, in_specs=specs, compiler_params=params, name=name, **more
        )(*operands)

    return call


def message(n, pairs, dtype=jnp.int16):
    return jax.ShapeDtypeStruct((n, pairs, 2, LANES), dtype)


def swap(x, axis):
    return lax.all_to_all(x, axis, split_axis=0, concat_axis=0, tiled=True)


def on_device(orbitals, kernel, partner_owner, partner_local):
    orb_dev, rows_x, width_y = orbitals.shape
    tasks = partner_local.shape[0]
    peers = Z * Y
    total = peers * orb_dev
    block = Y * tasks
    sides = width_y // LANES
    own_z, own_y = lax.axis_index("z").reshape(1), lax.axis_index("y").reshape(1)
    own_task = own_y * tasks + lax.axis_index("fft")
    both = np.concatenate(tables(width_y), axis=1)
    high = both.astype(jnp.bfloat16)
    low = (both - high.astype(np.float32)).astype(jnp.bfloat16)
    shape = (Z, Y // sides, sides, orb_dev // 2 + 1, 2, LANES)
    far = (orbitals, partner_owner[:, :, 0].T, partner_local.T)
    far = [pltpu.with_memory_space_constraint(x, pltpu.HBM) for x in far]
    names = pltpu.VMEM((2, tasks), jnp.int32)
    scratch = [pltpu.VMEM(orbitals.shape, orbitals.dtype), names, names]
    scratch.append(pltpu.SemaphoreType.DMA((rows_x // Z + 2,)))
    packed = jax.ShapeDtypeStruct(shape, jnp.bfloat16)
    packed = local(pack_kernel, packed, "pack", 3, pltpu.HBM, scratch_shapes=scratch)(
        own_z, own_y, own_task, *far
    )
    first = swap(packed.reshape(peers, *shape[3:]), ("z", "y"))
    outs = (
        message(Z, block // 2 + 1),
        jax.ShapeDtypeStruct((2, total, LANES), jnp.bfloat16),
        jax.ShapeDtypeStruct((2 * total // LANES, LANES), jnp.float32),
    )
    there, chosen, place = local(density_kernel, outs, "density", 1)(own_z, first)
    there = swap(there, "z")
    there = local(onward_kernel, message(block, Z + 1), "onward", 1)(own_y, there, kernel)
    there = swap(there, ("y", "fft"))
    back = local(transform_kernel, message(block, Z // 2 + 1), "potential", 1)(
        own_task, there, jnp.asarray(high), jnp.asarray(low)
    )
    back = swap(back, ("y", "fft"))
    back = swap(local(return_kernel, message(Z, block // 2 + 1), "return")(back), "z")
    home = local(exchange_kernel, message(peers, orb_dev // 2 + 1), "exchange")(
        back, chosen, place
    )
    home = swap(home, ("z", "y"))
    result = jax.ShapeDtypeStruct(orbitals.shape, jnp.float32)
    scratch = [pltpu.VMEM(orbitals.shape, jnp.float32), pltpu.SemaphoreType.DMA((rows_x // Z,))]
    spec = pl.BlockSpec(memory_space=pltpu.HBM)
    return local(home_kernel, result, "home", out_specs=spec, scratch_shapes=scratch)(home)


def solution(mesh):
    devices = mesh.devices.reshape(Z, Y, mesh.devices.shape[1])
    fine = Mesh(devices, ("z", "y", "fft"))
    orb = ("z", "y")
    in_specs = (P(orb, "fft", None), P("fft", None), P(orb, None, None), P(orb, None))
    out_specs = P(orb, "fft", None)
    return jax.shard_map(
        on_device, mesh=fine, in_specs=in_specs, out_specs=out_specs, check_vma=False
    )
```

```python
import math

import jax
import jax.numpy as jnp
import numpy as np
from jax import lax
from jax.experimental import pallas as pl
from jax.experimental.pallas import tpu as pltpu
from jax.sharding import Mesh
from jax.sharding import PartitionSpec as P

Z, Y = 16, 4
LANES = 128
TOP = 32767.0
STEPS = 128.0
FLOOR = 1e-37
KERNEL_LOW, KERNEL_HIGH = 0.02, 2.0
KERNEL_MID = 0.5 * (math.log(KERNEL_HIGH) + math.log(KERNEL_LOW))
KERNEL_STEP = 0.5 * (math.log(KERNEL_HIGH) - math.log(KERNEL_LOW)) / TOP


def tables(length):
    series = np.arange(length, dtype=np.int64)
    angle = (series[:, None] * series[None, :] % length) * (2.0 * math.pi / length)
    return np.cos(angle).astype(np.float32), np.sin(angle).astype(np.float32)


def level_of(largest):
    return jnp.ceil(jnp.log(jnp.maximum(largest, FLOOR)) * (STEPS / math.log(2.0))) + 1.0


def coded(values, level):
    share = jnp.sqrt(jnp.abs(values) * jnp.exp(level * (-math.log(2.0) / STEPS)))
    share = jnp.round(jnp.minimum(share, 1.0) * TOP)
    return jnp.where(values < 0, -share, share)


def decoded(codes, level):
    share = codes * (1.0 / TOP)
    return share * jnp.abs(share) * jnp.exp(level * (math.log(2.0) / STEPS))


def to_16(codes):
    return codes.astype(jnp.int32).astype(jnp.int16)


def from_16(codes):
    return codes.astype(jnp.int32).astype(jnp.float32)


def halves(a):
    high = a.astype(jnp.bfloat16)
    low = (a - high.astype(jnp.float32)).astype(jnp.bfloat16)
    return high, low


def mul(a, b):
    return jnp.dot(a, b, preferred_element_type=jnp.float32)


def mul3(a, b):
    return mul(a[0], b[0]) + (mul(a[0], b[1]) + mul(a[1], b[0]))


def lane_of(shape):
    return lax.broadcasted_iota(jnp.int32, shape, len(shape) - 1)


def tail_sum(ref):
    return jnp.sum(ref[:, ref.shape[1] - 1].astype(jnp.int32), axis=0)


def turned(ref):
    n, pairs, _, lanes = ref.shape
    codes = ref[:, : pairs - 1].astype(jnp.int32).reshape(n, (pairs - 1) * 2, lanes)
    codes = jnp.swapaxes(codes, 0, 1).reshape((pairs - 1) * 2, n // 2, 2, lanes)
    return codes.astype(jnp.int16)


def block_level(values):
    return level_of(jnp.max(jnp.max(jnp.abs(values), axis=1, keepdims=True), axis=2, keepdims=True))


def pack_kernel(z_ref, y_ref, task_ref, orb_hbm, owner_hbm, local_hbm, out_ref, *scratch):
    orb_ref, owner_ref, local_ref, sems = scratch
    loads = [
        pltpu.make_async_copy(source, here, sems.at[i])
        for i, (source, here) in enumerate(
            ((owner_hbm, owner_ref), (local_hbm, local_ref), (orb_hbm, orb_ref))
        )
    ]
    for load in loads:
        load.start()
    for load in loads:
        load.wait()
    count, rows, width = orb_ref.shape
    half = rows // Z
    orbs = orb_ref[...].astype(jnp.float32)
    for side in range(width // LANES):
        part = jnp.swapaxes(orbs[:, :, side * LANES : (side + 1) * LANES], 0, 1)
        for upper in range(half):
            piece = part[upper * Z : (upper + 1) * Z].reshape(Z, count // 2, 2, LANES)
            out_ref[:, upper, side, : count // 2] = piece.astype(jnp.bfloat16)
    names = (owner_ref[...] * count + local_ref[...] - 256).astype(jnp.float32)
    rest = jnp.zeros((2, LANES - names.shape[1]), jnp.float32)
    tail = jnp.concatenate([names, rest], axis=1).astype(jnp.bfloat16)
    shape = (Z, half, width // LANES, 1, 2, LANES)
    out_ref[:, :, :, count // 2 :] = jnp.broadcast_to(tail[None, None, None, None], shape)


def density_kernel(z_ref, first_ref, there_ref, chosen_ref, place_ref):
    peers, pairs, _, lanes = first_ref.shape
    pairs = pairs - 1
    total = peers * pairs * 2
    table = first_ref[:, :pairs].reshape(total, lanes)
    tasks = total // peers
    group = lanes // tasks
    tails = first_ref[:, pairs].astype(jnp.float32).reshape(peers // group, group, 2, lanes)
    place = tails[:, 0]
    for s in range(1, group):
        place = place + pltpu.roll(tails[:, s], s * tasks, 2)
    place = place.reshape(2 * (peers // group), lanes) + 256.0
    place_ref[...] = place
    column = place.T
    orbs = lane_of((lanes, total)).astype(jnp.float32)
    sides = []
    for c in range(2):
        pick = [
            (orbs == column[:, 2 * j + c : 2 * j + c + 1]).astype(jnp.bfloat16)
            for j in range(total // lanes)
        ]
        sides.append(mul(jnp.concatenate(pick, axis=0), table))
        chosen_ref[c] = sides[c].astype(jnp.bfloat16)
    n, block = there_ref.shape[0], there_ref.shape[1] - 1
    density = (sides[0] * sides[1]).reshape(n, 2 * block, lanes)
    level = block_level(density)
    there_ref[:, :block] = to_16(coded(density, level)).reshape(n, block, 2, lanes)
    shape = (n, 1, 2, lanes)
    tail = jnp.where(lane_of(shape) == z_ref[0], jnp.broadcast_to(level[:, None], shape), 0.0)
    there_ref[:, block:] = to_16(tail)


def onward_kernel(y_ref, there_ref, weight_ref, out_ref):
    depth, _, _, lanes = there_ref.shape
    block, half = out_ref.shape[0], depth // 2
    out_ref[:, :half] = turned(there_ref)
    tail = tail_sum(there_ref).astype(jnp.int16)
    out_ref[:, 2 * half :] = jnp.broadcast_to(tail[None, None], (block, 1, 2, lanes))
    own = jnp.zeros((depth, lanes), jnp.float32)
    halved = weight_ref.shape[1] // lanes
    for upper in range(weight_ref.shape[0] // depth):
        for side in range(halved):
            part = weight_ref[upper * depth : (upper + 1) * depth, side * lanes : (side + 1) * lanes]
            own = jnp.where(y_ref[0] == upper * halved + side, part, own)
    own = jnp.round((jnp.log(own) - KERNEL_MID) * (1.0 / KERNEL_STEP)).reshape(half, 2, lanes)
    out_ref[:, half : 2 * half] = jnp.broadcast_to(to_16(own)[None], (block, half, 2, lanes))


def transform_kernel(task_ref, data_ref, cs_high, cs_low, out_ref):
    n = cs_high.shape[0]
    count, _, _, lanes = data_ref.shape
    depth = n * n // (count * lanes)
    half = depth // 2
    halved = n // lanes

    def assembled(blocks):
        blocks = blocks.reshape(Y // halved, halved, count // Y, depth, lanes)
        sides = [
            jnp.concatenate(
                [blocks[upper, side][:, None] for upper in range(Y // halved)], axis=1
            ).reshape(n, lanes)
            for side in range(halved)
        ]
        return jnp.concatenate(sides, axis=1)

    codes = from_16(data_ref[:, :half].reshape(count, depth, lanes))
    tail = from_16(data_ref[:, 2 * half, :1])
    tail = jnp.broadcast_to(tail, (count, depth, lanes))
    row = lax.broadcasted_iota(jnp.int32, tail.shape, 1)
    tail = jnp.where(lane_of(tail.shape) == row, tail, 0.0)
    grid = assembled(decoded(codes, jnp.sum(tail, axis=2, keepdims=True)))
    log_weight = assembled(from_16(data_ref[:, half : 2 * half].reshape(count, depth, lanes)))
    weight = jnp.exp(log_weight * KERNEL_STEP + KERNEL_MID).T * (1.0 / (n * n))
    row = (cs_high[:, :], cs_low[:, :])
    cos = (cs_high[:, :n], cs_low[:, :n])
    sin = (cs_high[:, n:], cs_low[:, n:])
    u = halves(mul3(halves(grid), row))
    p = mul3(cos, u)
    q = mul3(sin, u)
    h_real = halves((p[:, :n] - q[:, n:]) * weight)
    h_imag = halves((p[:, n:] + q[:, :n]) * weight)
    g_real = halves(mul3(cos, h_real) + mul3(sin, h_imag))
    g_imag = halves(mul3(sin, h_real) - mul3(cos, h_imag))
    spread = mul3(g_real, cos) - mul3(g_imag, sin)
    level = level_of(jnp.max(jnp.abs(spread), axis=(0, 1), keepdims=True))
    codes = coded(spread, level).reshape(count // Y, Y // halved, depth, n)
    pair = jnp.full((2, lanes), task_ref[0] // 2, jnp.int32)
    side = lax.broadcasted_iota(jnp.int32, (2, lanes), 0)
    kept = (lane_of((2, lanes)) == pair) & (side == task_ref[0] % 2)
    tail = jnp.where(kept, level, 0.0)
    out_ref[:, half:] = to_16(jnp.broadcast_to(tail[None, None], (count, 1, 2, lanes)))
    for upper in range(Y // halved):
        for side in range(halved):
            part = codes[:, upper, :, side * lanes : (side + 1) * lanes]
            start = (upper * halved + side) * (count // Y)
            part = to_16(part).reshape(count // Y, half, 2, lanes)
            out_ref[start : start + count // Y, :half] = part


def return_kernel(back_ref, out_ref):
    half = out_ref.shape[1] - 1
    out_ref[:, :half] = turned(back_ref)
    tail = tail_sum(back_ref).astype(jnp.int16)
    out_ref[:, half:] = jnp.broadcast_to(tail[None, None], (out_ref.shape[0], 1, 2, tail.shape[1]))


def exchange_kernel(spread_ref, chosen_ref, place_ref, out_ref):
    total, lanes = chosen_ref.shape[1:]
    n, pairs = spread_ref.shape[0], spread_ref.shape[1] - 1
    tail = from_16(spread_ref[:, pairs])
    tail = jnp.broadcast_to(tail[:, None], (n, pairs, 2, lanes)).reshape(n, 2 * pairs, lanes)
    row = lax.broadcasted_iota(jnp.int32, tail.shape, 1)
    tail = jnp.where(lane_of(tail.shape) == row // 2, tail, 0.0).reshape(total, lanes)
    level = jnp.sum(tail, axis=1, keepdims=True)
    codes = from_16(spread_ref[:, :pairs].reshape(total, lanes))
    potential = decoded(codes, level)
    orbs = lax.broadcasted_iota(jnp.int32, (total, lanes), 0).astype(jnp.float32)
    summed = jnp.zeros((total, 2 * lanes), jnp.float32)
    for c in range(2):
        contrib = potential * chosen_ref[1 - c].astype(jnp.float32)
        high, low = halves(contrib)
        select = [
            (orbs == place_ref[2 * j + c : 2 * j + c + 1]).astype(jnp.bfloat16)
            for j in range(total // lanes)
        ]
        summed += mul(jnp.concatenate(select, axis=1), jnp.concatenate([high, low], axis=1))
    peers, half = out_ref.shape[0], out_ref.shape[1] - 1
    summed = -(summed[:, :lanes] + summed[:, lanes:]).reshape(peers, 2 * half, lanes)
    level = block_level(summed)
    out_ref[:, :half] = to_16(coded(summed, level)).reshape(peers, half, 2, lanes)
    out_ref[:, half:] = to_16(jnp.broadcast_to(level[:, None], (peers, 1, 2, lanes)))


def home_kernel(home_ref, out_hbm, out_ref, sems):
    count, rows, width = out_ref.shape
    peers, half = home_ref.shape[0], home_ref.shape[1] - 1
    codes = from_16(home_ref[:, :half].reshape(peers, 2 * half, LANES))
    values = decoded(codes, from_16(home_ref[:, half])[:, :1])
    values = values.reshape(Z, rows // Z, width // LANES, count, LANES)
    stores = []
    for upper in range(rows // Z):
        half = pl.ds(upper * Z, Z)
        for side in range(width // LANES):
            part = jnp.swapaxes(values[:, upper, side], 0, 1)
            lanes = pl.ds(side * LANES, LANES)
            out_ref[:, half, lanes] = part
            here, there = out_ref.at[:, half, lanes], out_hbm.at[:, half, lanes]
            stores.append(pltpu.make_async_copy(here, there, sems.at[len(stores)]))
            stores[-1].start()
    for store in stores:
        store.wait()


def local(kernel, out, name, scalars=0, arrays=pltpu.VMEM, **more):
    def call(*operands):
        specs = [pl.BlockSpec(memory_space=pltpu.SMEM)] * scalars
        specs += [pl.BlockSpec(memory_space=arrays)] * (len(operands) - scalars)
        params = pltpu.CompilerParams(vmem_limit_bytes=16 * 2**20)
        return pl.pallas_call(
            kernel, out_shape=out, in_specs=specs, compiler_params=params, name=name, **more
        )(*operands)

    return call


def message(n, pairs, dtype=jnp.int16):
    return jax.ShapeDtypeStruct((n, pairs, 2, LANES), dtype)


def swap(x, axis):
    return lax.all_to_all(x, axis, split_axis=0, concat_axis=0, tiled=True)


def on_device(orbitals, kernel, partner_owner, partner_local):
    orb_dev, rows_x, width_y = orbitals.shape
    tasks = partner_local.shape[0]
    peers = Z * Y
    total = peers * orb_dev
    block = Y * tasks
    sides = width_y // LANES
    own_z, own_y = lax.axis_index("z").reshape(1), lax.axis_index("y").reshape(1)
    own_task = own_y * tasks + lax.axis_index("fft")
    both = np.concatenate(tables(width_y), axis=1)
    high = both.astype(jnp.bfloat16)
    low = (both - high.astype(np.float32)).astype(jnp.bfloat16)
    shape = (Z, Y // sides, sides, orb_dev // 2 + 1, 2, LANES)
    far = (orbitals, partner_owner[:, :, 0].T, partner_local.T)
    far = [pltpu.with_memory_space_constraint(x, pltpu.HBM) for x in far]
    names = pltpu.VMEM((2, tasks), jnp.int32)
    scratch = [pltpu.VMEM(orbitals.shape, orbitals.dtype), names, names]
    scratch.append(pltpu.SemaphoreType.DMA((3,)))
    packed = jax.ShapeDtypeStruct(shape, jnp.bfloat16)
    packed = local(pack_kernel, packed, "pack", 3, pltpu.HBM, scratch_shapes=scratch)(
        own_z, own_y, own_task, *far
    )
    first = swap(packed.reshape(peers, *shape[3:]), ("z", "y"))
    outs = (
        message(Z, block // 2 + 1),
        jax.ShapeDtypeStruct((2, total, LANES), jnp.bfloat16),
        jax.ShapeDtypeStruct((2 * total // LANES, LANES), jnp.float32),
    )
    there, chosen, place = local(density_kernel, outs, "density", 1)(own_z, first)
    there = swap(there, "z")
    there = local(onward_kernel, message(block, Z + 1), "onward", 1)(own_y, there, kernel)
    there = swap(there, ("y", "fft"))
    back = local(transform_kernel, message(block, Z // 2 + 1), "potential", 1)(
        own_task, there, jnp.asarray(high), jnp.asarray(low)
    )
    back = swap(back, ("y", "fft"))
    back = swap(local(return_kernel, message(Z, block // 2 + 1), "return")(back), "z")
    home = local(exchange_kernel, message(peers, orb_dev // 2 + 1), "exchange")(
        back, chosen, place
    )
    home = swap(home, ("z", "y"))
    result = jax.ShapeDtypeStruct(orbitals.shape, jnp.float32)
    scratch = [pltpu.VMEM(orbitals.shape, jnp.float32), pltpu.SemaphoreType.DMA((Y,))]
    spec = pl.BlockSpec(memory_space=pltpu.HBM)
    return local(home_kernel, result, "home", out_specs=spec, scratch_shapes=scratch)(home)


def solution(mesh):
    devices = mesh.devices.reshape(Z, Y, mesh.devices.shape[1])
    fine = Mesh(devices, ("z", "y", "fft"))
    orb = ("z", "y")
    in_specs = (P(orb, "fft", None), P("fft", None), P(orb, None, None), P(orb, None))
    out_specs = P(orb, "fft", None)
    return jax.shard_map(
        on_device, mesh=fine, in_specs=in_specs, out_specs=out_specs, check_vma=False
    )
```
